512 devices in a mesh: orb: 32 (over x, y), grid: 16 (over z, core).
Axes of the slice: x: 4, y: 8, z: 8, core: 2. Of those that a mesh axis runs over, the one named last changes fastest.
Arguments:
- orbitals: float32 [128, 32, 4096], P('orb', 'grid'), may hold values from -6 to 6
- rotation: float32 [128, 128], replicated, may hold values from -0.5 to 0.5
- tile_list: int32 [64, 2], replicated, may hold values from 0 to 31, as said below
- pair_mask: int32 [128, 128], replicated, may hold values from 0 to 1, as said below
Outputs:
- exchange_term: float32 [128, 32, 4096], P('orb', 'grid')
The draws below stay inside these ranges and needn't reach their ends.
Inputs may be any that keep to these rules, and one draw needn't show every extreme that they name: `tile_list`: row t names one tile: its target block and its source block of 4 orbitals each; no tile is named twice. `pair_mask`: among the 1024 orbital pairs that lie in listed tiles, exactly 512 are 1.
All inputs are finite; a program needn't handle non-finite values.
Results may differ from the reference program's by a relative error of at most 0.0003.
Values sent between devices are 32-bit elements; how exact they have to be, the bound alone decides.
A program may use at most 64 MiB of HBM per device.

```python
import jax
import jax.numpy as jnp
from jax import lax

NORB = 128
BLK = 4
NX = 32
NY = 64
NZ = 64
NB = 32
NPAIR = 1024
TILES = 64
LIVE = 512
N_ORB = 32


def tile_draw(key):
    shuffled = jax.random.permutation(jax.random.fold_in(key, 11), NB * NB)
    chosen = shuffled[:TILES].astype(jnp.int32)
    return jnp.stack([chosen // NB, chosen % NB], axis=1).astype(jnp.int32)


def draw_tile_list(key, part):
    return tile_draw(key)


def draw_pair_mask(key, part):
    tiles = tile_draw(key)
    within = jnp.arange(BLK * BLK, dtype=jnp.int32)
    targets = (BLK * tiles[:, 0:1] + within[None, :] // BLK).reshape(-1)
    sources = (BLK * tiles[:, 1:2] + within[None, :] % BLK).reshape(-1)
    background = jax.random.randint(jax.random.fold_in(key, 12), (NORB, NORB), 0, 2).astype(jnp.int32)
    shuffled = jax.random.permutation(jax.random.fold_in(key, 13), NPAIR)
    live_flags = jnp.zeros((NPAIR,), jnp.int32).at[shuffled[:LIVE]].set(1)
    return background.at[targets, sources].set(live_flags).astype(jnp.int32)


def steps_of(own_key, dims, pieces, low, top_value):
    level, own = 1.0, jax.random.fold_in(own_key, 6)
    for axis_at, parts in pieces:
        heights = jnp.exp(jax.random.uniform(jax.random.fold_in(own, axis_at), (parts,), jnp.float32, low / len(pieces), top_value / len(pieces)))
        level = level * jnp.repeat(heights, dims[axis_at] // parts).reshape([-1 if axis == axis_at else 1 for axis in range(len(dims))])
    return level


def scatter_about(rng, extent, spread, bound, split=(), kind=jnp.bfloat16):
    factor_of = steps_of(rng, extent, split, -0.22, 0.18) if split else 1.0
    entries = jax.random.normal(rng, extent, jnp.float32) * spread * factor_of
    return jnp.minimum(jnp.maximum(entries, -bound), bound).astype(kind)


def setup_inputs(seed: int = 0) -> dict:
    key_list = jax.random.split(jax.random.key(seed), 5)
    orbitals = scatter_about(key_list[0], (NORB, NX, NY * NZ), 1.0, 6.0, ((0, 32), (1, 16)), jnp.float32)
    rotation = scatter_about(key_list[1], (NORB, NORB), NORB ** -0.5, 0.5, (), jnp.float32)
    tile_list = draw_tile_list(jax.random.fold_in(key_list[4], 71), 0)
    pair_mask = draw_pair_mask(jax.random.fold_in(key_list[4], 71), 0)
    return dict(orbitals=orbitals, rotation=rotation, tile_list=tile_list, pair_mask=pair_mask)


precise = lax.Precision.HIGHEST
coupling = 0.25
screening = 0.1

def sine_table(length):
    wave_index = jnp.arange(length, dtype=jnp.float32) + 1.0
    return jnp.sqrt(2.0 / (length + 1.0)) * jnp.sin(jnp.pi * wave_index[:, None] * wave_index[None, :] / (length + 1.0))

def eigen_values(length):
    wave_index = jnp.arange(length, dtype=jnp.float32) + 1.0
    return 2.0 - 2.0 * jnp.cos(jnp.pi * wave_index / (length + 1.0))

def green_kernel(size_x, size_y, size_z):
    summed = eigen_values(size_x)[:, None, None] + eigen_values(size_y)[None, :, None] + eigen_values(size_z)[None, None, :]
    return coupling / (summed + screening)

def pair_lists(tile_list, pair_mask):
    within = jnp.arange(BLK * BLK, dtype=jnp.int32)
    targets = (BLK * tile_list[:, 0:1] + within[None, :] // BLK).reshape(-1).astype(jnp.int32)
    sources = (BLK * tile_list[:, 1:2] + within[None, :] % BLK).reshape(-1).astype(jnp.int32)
    return (targets, sources, pair_mask[targets, sources])

def compact(targets, sources, live_flags, number):
    ranking = (jnp.cumsum(live_flags) - 1).astype(jnp.int32)
    places = jnp.where(live_flags == 1, ranking, number).astype(jnp.int32)
    picked = jnp.zeros((number,), jnp.int32).at[places].set(jnp.arange(live_flags.shape[0], dtype=jnp.int32), mode='drop')
    return (targets[picked], sources[picked])

def transform_all(values, matrix_x, matrix_y, matrix_z):
    values = jnp.einsum('gxyz,zk->gxyk', values, matrix_z, precision=precise)
    values = jnp.einsum('gxyz,yk->gxkz', values, matrix_y, precision=precise)
    return jnp.einsum('gxyz,xk->gkyz', values, matrix_x, precision=precise)

def reference(orbitals, rotation, tile_list, pair_mask):
    rotated = jnp.einsum('ij,ixc->jxc', rotation, orbitals, precision=precise).reshape(NORB, NX, NY, NZ)
    targets, sources, live_flags = pair_lists(tile_list, pair_mask)
    targets, sources = compact(targets, sources, live_flags, LIVE)
    targets = targets.reshape(N_ORB, -1)
    sources = sources.reshape(N_ORB, -1)
    matrix_x = sine_table(NX)
    matrix_y = sine_table(NY)
    matrix_z = sine_table(NZ)
    kernel = green_kernel(NX, NY, NZ)

    def accumulate(carry, pair_group):
        group_targets, group_sources = pair_group
        density = rotated[group_targets] * rotated[group_sources]
        spectrum = transform_all(density, matrix_x, matrix_y, matrix_z) * kernel
        potential = transform_all(spectrum, matrix_x, matrix_y, matrix_z)
        products = potential * rotated[group_sources]
        selector = (group_targets[:, None] == jnp.arange(NORB, dtype=jnp.int32)[None, :]).astype(jnp.float32)
        return (carry - jnp.einsum('gi,gxyz->ixyz', selector, products, precision=precise), None)
    start = jnp.zeros((NORB, NX, NY, NZ), jnp.float32)
    summed, ignored = lax.scan(accumulate, start, (targets, sources))
    return summed.reshape(NORB, NX, NY * NZ)
```

```python
import numpy as np
import jax
import jax.numpy as jnp
from jax import lax
from jax.experimental import pallas as pl
from jax.experimental.pallas import tpu as pltpu
from jax.sharding import PartitionSpec as P

NORB = 128
NX = 32
NY = 64
NZ = 64
NPAIR = 1024
LANES = 128
N_ORB = 32
N_GRID = 16
XDIM = 4
YDIM = 8
ZDIM = 8
ROWS = 1024
PREP = 256
coupling = 0.25
screening = 0.1
MESH = pl.DeviceIdType.MESH
f32 = jnp.float32
bf16 = jnp.bfloat16


def sine_table(length):
    k = np.arange(length, dtype=np.float64) + 1.0
    return np.sqrt(2.0 / (length + 1.0)) * np.sin(np.pi * k[:, None] * k[None, :] / (length + 1.0))


def eigen_values(length):
    k = np.arange(length, dtype=np.float64) + 1.0
    return 2.0 - 2.0 * np.cos(np.pi * k / (length + 1.0))


def halves(table):
    high = table.astype(np.float32).astype(jnp.bfloat16)
    low = (table - high.astype(np.float64)).astype(np.float32).astype(jnp.bfloat16)
    return high, low


def tables():
    sx_h, sx_l = halves(sine_table(NX))
    table_x = np.concatenate([sx_h, sx_h, sx_l], axis=1)
    s = sine_table(NY)
    split_cols = np.concatenate([s[:, 0::2], s[:, 1::2]], axis=1)
    fh, fl = halves(split_cols)
    table_yf = np.concatenate([fh, fh, fl], axis=1)
    ih, il = halves(split_cols.T)
    table_yi = np.concatenate([ih, ih, il], axis=1)
    block = np.kron(np.eye(2), sine_table(NZ))
    bh, bl = halves(block)
    table_z = np.concatenate([bh, bl], axis=1)
    ly, lz, lx = eigen_values(NY), eigen_values(NZ), eigen_values(NX)
    sum_yz = ly[:, None] + np.tile(lz, 2)[None, :] + screening
    sum_x = np.repeat(lx.reshape(NX // 2, 2), NZ, axis=1)
    return (
        table_x,
        table_yf,
        table_yi,
        table_z,
        sum_yz.astype(np.float32),
        sum_x.astype(np.float32),
    )


def split(v):
    high = v.astype(bf16)
    low = (v - high.astype(f32)).astype(bf16)
    return high, low


def dot(a, b):
    return jnp.dot(a, b, preferred_element_type=f32)


def dot_nt(a, b):
    return lax.dot_general(a, b, (((1,), (1,)), ((), ())), preferred_element_type=f32)


def iota(shape, dim):
    return lax.broadcasted_iota(jnp.int32, shape, dim)


def one_hot(cond):
    return jnp.where(cond, 1.0, 0.0).astype(bf16)


def z_product(v, table_z):
    high, low = split(v)
    a = dot(high, table_z)
    return a[:, :LANES] + a[:, LANES:] + dot(low, table_z[:, :LANES])


def kernel(
    orb_ref, rotation_ref, tile_ref, mask_ref, tx_ref, tyf_ref, tyi_ref, tz_ref, syz_ref, sx_ref,
    out_ref,
    own, got, sel_i, sel_j, sel_t, rot_k, rot_j, green, dens,
    ra, rb, box, mid, pot, ra2, rb2, back, term, gathered,
    in_sem, out_sem,
    e1_s, e1_r, a1_s, a1_r, b1_s, b1_r, a2_s, b2_s, x_ra, x_rb,
    c1_s, c1_r, d1_s, d1_r, c2_s, c2_r, d2_s, d2_r, e4_s, e4_r,
):
    o = lax.axis_index("orb")
    g = lax.axis_index("grid")
    x, y = o // YDIM, o % YDIM
    z, c = g // 2, g % 2

    def orb_peer(d):
        return ((x + d // YDIM) % XDIM) * YDIM + (y + d % YDIM) % YDIM

    def to_orb(src, dst, s_sem, r_sem, o2):
        return pltpu.make_async_remote_copy(
            src_ref=src, dst_ref=dst, send_sem=s_sem, recv_sem=r_sem,
            device_id=(o2, g), device_id_type=MESH,
        )

    def to_grid(src, dst, s_sem, r_sem, g2):
        return pltpu.make_async_remote_copy(
            src_ref=src, dst_ref=dst, send_sem=s_sem, recv_sem=r_sem,
            device_id=(o, g2), device_id_type=MESH,
        )

    def arrived(ref, sem):
        pltpu.make_async_copy(ref, ref, sem).wait()

    def orb_order(d):
        return (d * 11) % N_ORB

    def z_order(d):
        return (z + (d * 3) % ZDIM) % ZDIM

    for k in range(4):
        pltpu.make_async_copy(orb_ref.at[k], own.at[pl.ds(2 * k, 2), :], in_sem.at[k]).start()
    barrier = pltpu.get_barrier_semaphore()

    @pl.loop(1, N_ORB)
    def _(d):
        pl.semaphore_signal(barrier, inc=1, device_id=(orb_peer(d), g), device_id_type=MESH)

    @pl.loop(1, N_GRID)
    def _(d):
        g2 = ((z + d // 2) % ZDIM) * 2 + (c + d) % 2
        pl.semaphore_signal(barrier, inc=1, device_id=(o, g2), device_id_type=MESH)

    for k in range(4):
        pltpu.make_async_copy(orb_ref.at[k], own.at[pl.ds(2 * k, 2), :], in_sem.at[k]).wait()
    pl.semaphore_wait(barrier, N_ORB - 1 + N_GRID - 1)

    def cells(o2):
        return pl.ds(pl.multiple_of(o2 * LANES, LANES), LANES)

    pltpu.make_async_copy(own.at[:, cells(o)], got.at[o], e1_r).start()

    @pl.loop(1, N_ORB)
    def _(d):
        o2 = orb_peer(orb_order(d))
        to_orb(own.at[:, cells(o2)], got.at[o], e1_s, e1_r, o2).start()

    tiles = tile_ref[...].astype(f32)
    p_lane = iota((64, NPAIR), 1)
    in_tile = p_lane // 16 == iota((64, NPAIR), 0)
    p_row = iota((1, NPAIR), 1)
    target = 4.0 * jnp.sum(jnp.where(in_tile, tiles[:, 0:1], 0.0), axis=0, keepdims=True)
    target = target + (p_row // 4 % 4).astype(f32)
    source = 4.0 * jnp.sum(jnp.where(in_tile, tiles[:, 1:2], 0.0), axis=0, keepdims=True)
    source = source + (p_row % 4).astype(f32)
    half = (iota((256, NPAIR), 0) // 2).astype(f32)
    hot_i = one_hot(half == target)
    hot_j = one_hot(half == source)
    orb_row = iota((NORB, NPAIR), 0).astype(f32)
    mask_of = dot(mask_ref[...].astype(f32).astype(bf16), one_hot(orb_row == source))
    live = jnp.sum(jnp.where(orb_row == target, mask_of, 0.0), axis=0, keepdims=True)
    before = one_hot(iota((LANES, LANES), 0) < iota((LANES, LANES), 1))
    every = jnp.ones((LANES, LANES), bf16)
    running = jnp.zeros((8, LANES), f32)
    ranks = []
    for k in range(NPAIR // LANES):
        flags = jnp.broadcast_to(live[:, k * LANES : (k + 1) * LANES], (8, LANES))
        bits = flags.astype(bf16)
        rank = dot(bits, before) + running
        running = running + dot(bits, every)
        ranks.append(jnp.where(flags > 0.5, rank, -1.0)[0:1, :])
    rank = jnp.concatenate(ranks, axis=1)

    same_plane = iota((PREP, 256), 0) % 2 == iota((PREP, 256), 1) % 2

    def select_rows(r, carry):
        rows = pl.ds(pl.multiple_of(r * PREP, PREP), PREP)
        slot = ((iota((PREP, NPAIR), 0) + r * PREP) // 2).astype(f32)
        chosen = one_hot(slot == rank)
        sel_i[rows, :] = jnp.where(same_plane, dot_nt(chosen, hot_i), 0.0).astype(bf16)
        sel_j[rows, :] = jnp.where(same_plane, dot_nt(chosen, hot_j), 0.0).astype(bf16)
        sel_t[r] = jnp.where(same_plane, dot_nt(hot_i, chosen), 0.0).astype(bf16)
        return carry

    lax.fori_loop(0, ROWS // PREP, select_rows, 0)

    widen = one_hot(iota((256, NORB), 0) // 2 == iota((256, NORB), 1))
    widen_t = one_hot(iota((NORB, 256), 0) == iota((NORB, 256), 1) // 2)
    for k, part in enumerate(split(rotation_ref[...])):
        tall = dot_nt(widen, part).astype(bf16)
        rot_k[k] = jnp.where(same_plane, dot(tall, widen_t), 0.0).astype(bf16)

    def fill_green(k, carry):
        green[k] = coupling / (syz_ref[...] + sx_ref[pl.ds(k, 1), :])
        return carry

    lax.fori_loop(0, NX // 2, fill_green, 0)

    arrived(got, e1_r)

    got_h, got_l = split(got[...].reshape(256, LANES))
    rotated = dot(rot_k[0], got_h) + dot(rot_k[0], got_l) + dot(rot_k[1], got_h)
    rotated = jnp.concatenate(split(rotated), axis=1)

    def density_rows(r, carry):
        rows = pl.ds(pl.multiple_of(r * 128, 128), 128)
        wide_i = dot(sel_i[rows, :], rotated)
        wide_j = dot(sel_j[rows, :], rotated)
        at_j = wide_j[:, :LANES] + wide_j[:, LANES:]
        rot_j[rows, :] = at_j
        density = (wide_i[:, :LANES] + wide_i[:, LANES:]) * at_j
        spectrum = z_product(density, tz_ref[...])
        dens[pl.ds(r * 4, 4)] = spectrum.reshape(4, 32, LANES)
        return carry

    lax.fori_loop(0, ROWS // 128, density_rows, 0)

    ours = pl.ds(2 * g, 2)

    def z_rows(z2):
        return pl.ds(2 * z2, 2)

    def z_rows_b(z2):
        return pl.ds(16 + 2 * z2, 2)

    pltpu.make_async_copy(dens.at[o, pl.ds(0, 16), :], ra.at[o], a1_r).start()

    @pl.loop(1, N_ORB)
    def _(d):
        o2 = orb_peer(orb_order(d))
        to_orb(dens.at[o2, pl.ds(0, 16), :], ra.at[o], a1_s, a1_r, o2).start()

    @pl.when(c == 1)
    def _():
        pltpu.make_async_copy(dens.at[:, z_rows_b(z), :], rb.at[:, ours, :], b1_r).start()

    @pl.when(c == 0)
    def _():
        to_grid(dens.at[:, z_rows_b(z), :], rb.at[:, ours, :], b1_s, b1_r, 2 * z + 1).start()

    @pl.loop(1, ZDIM)
    def _(d):
        z2 = z_order(d)
        to_grid(dens.at[:, z_rows_b(z2), :], rb.at[:, ours, :], b1_s, b1_r, 2 * z2 + 1).start()

    arrived(ra, a1_r)

    @pl.when(c == 0)
    def _():
        pltpu.make_async_copy(ra.at[:, z_rows(z), :], box.at[:, ours, :], x_ra).start()

    @pl.when(c == 1)
    def _():
        to_grid(ra.at[:, z_rows(z), :], box.at[:, ours, :], a2_s, x_ra, 2 * z).start()

    @pl.loop(1, ZDIM)
    def _(d):
        z2 = z_order(d)
        to_grid(ra.at[:, z_rows(z2), :], box.at[:, ours, :], a2_s, x_ra, 2 * z2).start()

    @pl.when(c == 1)
    def _():
        arrived(rb, b1_r)
        pltpu.make_async_copy(rb.at[o], box.at[o], x_rb).start()

        @pl.loop(1, N_ORB)
        def _(d):
            o2 = orb_peer(orb_order(d))
            to_orb(rb.at[o2], box.at[o], b2_s, x_rb, o2).start()

        arrived(box, x_rb)

    @pl.when(c == 0)
    def _():
        arrived(box, x_ra)

    def along_x(src, dst):
        def step(r, carry):
            v = src[pl.ds(r * 4, 4)]
            v = jnp.concatenate([v[k] for k in range(4)], axis=1)
            high, low = split(v)
            w = dot(tx_ref[...], jnp.concatenate([high, low, high], axis=0))
            for k in range(4):
                dst[pl.ds(pl.multiple_of((r * 4 + k) * NX, NX), NX), :] = w[:, k * LANES : (k + 1) * LANES]
            return carry

        lax.fori_loop(0, N_ORB // 4, step, 0)

    along_x(box, mid)
    low_half = iota((N_ORB, LANES), 1) < NZ

    for k in range(NX // 2):
        v0 = mid[pl.ds(2 * k, N_ORB, stride=NX), :]
        v1 = mid[pl.ds(2 * k + 1, N_ORB, stride=NX), :]
        even = jnp.where(low_half, v0, pltpu.roll(v1, NZ, 1))
        odd = jnp.where(low_half, pltpu.roll(v0, NZ, 1), v1)
        high, low = split(jnp.concatenate([even, odd], axis=0))
        spectrum = dot(tyf_ref[...], jnp.concatenate([high, low, high], axis=0)) * green[k]
        high, low = split(spectrum)
        w = dot(tyi_ref[...], jnp.concatenate([high, low, high], axis=0))
        even, odd = w[:N_ORB], w[N_ORB:]
        mid[pl.ds(2 * k, N_ORB, stride=NX), :] = jnp.where(low_half, even, pltpu.roll(odd, NZ, 1))
        mid[pl.ds(2 * k + 1, N_ORB, stride=NX), :] = jnp.where(low_half, pltpu.roll(even, NZ, 1), odd)

    def back_x(r, carry):
        v = jnp.concatenate(
            [mid[pl.ds(pl.multiple_of((r * 4 + k) * NX, NX), NX), :] for k in range(4)], axis=1
        )
        high, low = split(v)
        w = dot(tx_ref[...], jnp.concatenate([high, low, high], axis=0))
        for k in range(4):
            pot[r * 4 + k] = w[:, k * LANES : (k + 1) * LANES]
        return carry

    lax.fori_loop(0, N_ORB // 4, back_x, 0)

    @pl.when(c == 0)
    def _():
        pltpu.make_async_copy(pot.at[:, ours, :], ra2.at[:, z_rows(z), :], c1_r).start()

        @pl.loop(1, N_GRID)
        def _(d):
            g2 = ((z + (d // 2) * 3) % ZDIM) * 2 + (c + d) % 2
            to_grid(pot.at[:, pl.ds(2 * g2, 2), :], ra2.at[:, z_rows(z), :], c1_s, c1_r, g2).start()

    @pl.when(c == 1)
    def _():
        pltpu.make_async_copy(pot.at[o], rb2.at[o], d1_r).start()

        @pl.loop(1, N_ORB)
        def _(d):
            o2 = orb_peer(orb_order(d))
            to_orb(pot.at[o2], rb2.at[o], d1_s, d1_r, o2).start()

    arrived(ra2, c1_r)
    pltpu.make_async_copy(ra2.at[o], back.at[o, pl.ds(0, 16), :], c2_r).start()

    @pl.loop(1, N_ORB)
    def _(d):
        o2 = orb_peer(orb_order(d))
        to_orb(ra2.at[o2], back.at[o, pl.ds(0, 16), :], c2_s, c2_r, o2).start()

    @pl.when(c == 1)
    def _():
        arrived(rb2, d1_r)
        pltpu.make_async_copy(rb2.at[:, ours, :], back.at[:, z_rows_b(z), :], d2_r).start()

        @pl.loop(1, N_GRID)
        def _(d):
            g2 = ((z + (d // 2) * 3) % ZDIM) * 2 + (c + d) % 2
            to_grid(rb2.at[:, pl.ds(2 * g2, 2), :], back.at[:, z_rows_b(z), :], d2_s, d2_r, g2).start()

    arrived(back.at[:, pl.ds(0, 16), :], c2_r)
    arrived(back.at[:, pl.ds(16, 16), :], d2_r)

    total = jnp.zeros((256, 2 * LANES), f32)
    for r in range(ROWS // PREP):
        rows = pl.ds(r * PREP, PREP)
        potential = z_product(back[pl.ds(r * 8, 8)].reshape(PREP, LANES), tz_ref[...])
        products = jnp.concatenate(split(potential * rot_j[rows, :]), axis=1)
        total = total + dot(sel_t[r], products)
    term[...] = (-(total[:, :LANES] + total[:, LANES:])).reshape(N_ORB, 8, LANES)

    pltpu.make_async_copy(term.at[o], gathered.at[:, cells(o)], e4_r).start()

    @pl.loop(1, N_ORB)
    def _(d):
        o2 = orb_peer(orb_order(d))
        to_orb(term.at[o2], gathered.at[:, cells(o)], e4_s, e4_r, o2).start()

    most = pl.ds(0, N_ORB - 1)
    arrived(got.at[most], e1_s)
    arrived(ra.at[most], a1_s)
    arrived(term.at[most], e4_s)
    arrived(ra2.at[most], c2_s)

    @pl.when(c == 0)
    def _():
        arrived(rb.at[:, pl.ds(0, 16), :], b1_s)
        arrived(ra.at[:, pl.ds(0, 14), :], a2_s)
        arrived(pot.at[:, pl.ds(0, 30), :], c1_s)

    @pl.when(c == 1)
    def _():
        arrived(rb.at[:, pl.ds(0, 14), :], b1_s)
        arrived(ra.at[:, pl.ds(0, 16), :], a2_s)
        arrived(rb.at[most], b2_s)
        arrived(pot.at[most], d1_s)
        arrived(rb2.at[:, pl.ds(0, 30), :], d2_s)

    arrived(gathered, e4_r)
    for k in range(4):
        pltpu.make_async_copy(gathered.at[pl.ds(2 * k, 2), :], out_ref.at[k], out_sem.at[k]).start()
    for k in range(4):
        pltpu.make_async_copy(gathered.at[pl.ds(2 * k, 2), :], out_ref.at[k], out_sem.at[k]).wait()


def on_device(orbitals, rotation, tile_list, pair_mask):
    consts = [jnp.asarray(t) for t in tables()]
    vmem = pl.BlockSpec(memory_space=pltpu.VMEM)
    anyspace = pl.BlockSpec(memory_space=pl.ANY)
    dma = pltpu.SemaphoreType.DMA
    box = pltpu.VMEM((N_ORB, NX, LANES), f32)
    half_box = pltpu.VMEM((N_ORB, 16, LANES), f32)
    return pl.pallas_call(
        kernel,
        out_shape=jax.ShapeDtypeStruct(orbitals.shape, f32),
        in_specs=[anyspace] + [vmem] * (3 + len(consts)),
        out_specs=anyspace,
        scratch_shapes=[
            pltpu.VMEM((8, NY * NZ), f32),
            pltpu.VMEM((N_ORB, 8, LANES), f32),
            pltpu.VMEM((ROWS, 256), bf16),
            pltpu.VMEM((ROWS, 256), bf16),
            pltpu.VMEM((ROWS // PREP, 256, PREP), bf16),
            pltpu.VMEM((2, 256, 256), bf16),
            pltpu.VMEM((ROWS, LANES), f32),
            pltpu.VMEM((NX // 2, NY, LANES), f32),
            box,
            half_box,
            box,
            box,
            pltpu.VMEM((N_ORB * NX, LANES), f32),
            box,
            half_box,
            box,
            box,
            pltpu.VMEM((N_ORB, 8, LANES), f32),
            pltpu.VMEM((8, NY * NZ), f32),
            dma((4,)),
            dma((4,)),
        ]
        + [dma] * 20,
        compiler_params=pltpu.CompilerParams(
            collective_id=0, has_side_effects=True, vmem_limit_bytes=48 * 2**20
        ),
    )(orbitals, rotation, tile_list, pair_mask, *consts)


def solution(mesh):
    in_specs = (P("orb", "grid", None), P(), P(), P())
    out_specs = P("orb", "grid", None)
    return jax.shard_map(
        on_device, mesh=mesh, in_specs=in_specs, out_specs=out_specs, check_vma=False
    )
```

```python
import numpy as np
import jax
import jax.numpy as jnp
from jax import lax
from jax.experimental import pallas as pl
from jax.experimental.pallas import tpu as pltpu
from jax.sharding import PartitionSpec as P

NORB = 128
NX = 32
NY = 64
NZ = 64
NPAIR = 1024
LANES = 128
N_ORB = 32
N_GRID = 16
XDIM = 4
YDIM = 8
ZDIM = 8
DX = (2, 1, 3, 0)
ROWS = 1024
PREP = 256
coupling = 0.25
screening = 0.1
MESH = pl.DeviceIdType.MESH
f32 = jnp.float32
bf16 = jnp.bfloat16


def sine_table(length):
    k = np.arange(length, dtype=np.float64) + 1.0
    return np.sqrt(2.0 / (length + 1.0)) * np.sin(np.pi * k[:, None] * k[None, :] / (length + 1.0))


def eigen_values(length):
    k = np.arange(length, dtype=np.float64) + 1.0
    return 2.0 - 2.0 * np.cos(np.pi * k / (length + 1.0))


def halves(table):
    high = table.astype(np.float32).astype(jnp.bfloat16)
    low = (table - high.astype(np.float64)).astype(np.float32).astype(jnp.bfloat16)
    return high, low


def tables():
    sx_h, sx_l = halves(sine_table(NX))
    table_x = np.concatenate([sx_h, sx_h, sx_l], axis=1)
    s = sine_table(NY)
    split_cols = np.concatenate([s[:, 0::2], s[:, 1::2]], axis=1)
    fh, fl = halves(split_cols)
    table_yf = np.concatenate([fh, fh, fl], axis=1)
    ih, il = halves(split_cols.T)
    table_yi = np.concatenate([ih, ih, il], axis=1)
    block = np.kron(np.eye(2), sine_table(NZ))
    bh, bl = halves(block)
    table_z = np.concatenate([bh, bl], axis=1)
    ly, lz, lx = eigen_values(NY), eigen_values(NZ), eigen_values(NX)
    sum_yz = ly[:, None] + np.tile(lz, 2)[None, :] + screening
    sum_x = np.repeat(lx.reshape(NX // 2, 2), NZ, axis=1)
    return (
        table_x,
        table_yf,
        table_yi,
        table_z,
        sum_yz.astype(np.float32),
        sum_x.astype(np.float32),
    )


def split(v):
    high = v.astype(bf16)
    low = (v - high.astype(f32)).astype(bf16)
    return high, low


def dot(a, b):
    return jnp.dot(a, b, preferred_element_type=f32)


def dot_nt(a, b):
    return lax.dot_general(a, b, (((1,), (1,)), ((), ())), preferred_element_type=f32)


def iota(shape, dim):
    return lax.broadcasted_iota(jnp.int32, shape, dim)


def one_hot(cond):
    return jnp.where(cond, 1.0, 0.0).astype(bf16)


def z_product(v, table_z):
    high, low = split(v)
    a = dot(high, table_z)
    return a[:, :LANES] + a[:, LANES:] + dot(low, table_z[:, :LANES])


def kernel(
    orb_hbm, rotation_hbm, tile_hbm, mask_hbm, tx_hbm, tyf_hbm, tyi_hbm, tz_hbm, syz_hbm, sx_hbm,
    out_ref,
    rotation_ref, tile_ref, mask_ref, tx_ref, tyf_ref, tyi_ref, tz_ref, syz_ref, sx_ref,
    own, got, sel_i, sel_j, sel_t, rot_k, rot_j, green, dens,
    ra, rb, box, mid, pot, ra2, rb2, back, term, gathered,
    in_sem, out_sem, table_sem,
    a1_r, b1_r, x_ra, x_rb, c1_r, d1_r, c2_r, d2_r,
    e1_r, e4_r, e1_s, a1_s, b1_s, a2_s, b2_s, c1_s, d1_s, c2_s, d2_s, e4_s,
):
    o = lax.axis_index("orb")
    g = lax.axis_index("grid")
    x, y = o // YDIM, o % YDIM
    z, c = g // 2, g % 2

    def step_of(i):
        return (YDIM - i) // 2 * (1 - 2 * (i % 2))

    def ahead(j, i):
        return (x + DX[j]) % XDIM * YDIM + (y + YDIM + step_of(i)) % YDIM

    def behind(j, i):
        return (x + XDIM - DX[j]) % XDIM * YDIM + (y + YDIM - step_of(i)) % YDIM

    def block(j):
        return pl.ds(pl.multiple_of((x + DX[j]) % XDIM * YDIM, YDIM), YDIM)

    def chunk(j):
        return pl.ds(j * YDIM, YDIM)

    def z_peer(i):
        return (z + ZDIM + step_of(i)) % ZDIM

    def peers(j):
        return YDIM - 1 if DX[j] == 0 else YDIM

    def to_orb(src, dst, s_sem, r_sem, o2):
        pltpu.make_async_remote_copy(
            src_ref=src, dst_ref=dst, send_sem=s_sem, recv_sem=r_sem,
            device_id=(o2, g), device_id_type=MESH,
        ).start()

    def to_grid(src, dst, s_sem, r_sem, g2):
        pltpu.make_async_remote_copy(
            src_ref=src, dst_ref=dst, send_sem=s_sem, recv_sem=r_sem,
            device_id=(o, g2), device_id_type=MESH,
        ).start()

    def here(src, dst, r_sem):
        pltpu.make_async_copy(src, dst, r_sem).start()

    def arrived(ref, sem):
        pltpu.make_async_copy(ref, ref, sem).wait()

    loads = [
        (orb_hbm.at[n], own.at[pl.ds(2 * n, 2), :], in_sem.at[n]) for n in range(4)
    ]
    fetches = [
        (tile_hbm, tile_ref), (mask_hbm, mask_ref), (rotation_hbm, rotation_ref),
        (syz_hbm, syz_ref), (sx_hbm, sx_ref), (tz_hbm, tz_ref),
        (tx_hbm, tx_ref), (tyf_hbm, tyf_ref), (tyi_hbm, tyi_ref),
    ]
    for args in loads:
        pltpu.make_async_copy(*args).start()
    for n, (src, dst) in enumerate(fetches):
        pltpu.make_async_copy(src, dst, table_sem.at[n]).start()
    barrier = pltpu.get_barrier_semaphore()
    for j in range(XDIM):

        @pl.loop(0, peers(j))
        def _(i):
            pl.semaphore_signal(barrier, inc=1, device_id=(ahead(j, i), g), device_id_type=MESH)

    @pl.loop(0, ZDIM - 1)
    def _(i):
        pl.semaphore_signal(barrier, inc=1, device_id=(o, 2 * z_peer(i)), device_id_type=MESH)
        pl.semaphore_signal(barrier, inc=1, device_id=(o, 2 * z_peer(i) + 1), device_id_type=MESH)

    pl.semaphore_signal(barrier, inc=1, device_id=(o, 2 * z + 1 - c), device_id_type=MESH)
    for args in loads:
        pltpu.make_async_copy(*args).wait()
    pl.semaphore_wait(barrier, N_ORB - 1 + N_GRID - 1)

    def cells(o2):
        return pl.ds(pl.multiple_of(o2 * LANES, LANES), LANES)

    for j in range(XDIM):

        @pl.loop(0, peers(j))
        def _(i):
            o2 = ahead(j, i)
            to_orb(own.at[:, cells(o2)], got.at[o], e1_s, e1_r, o2)

    here(own.at[:, cells(o)], got.at[o], e1_r)

    for n, (src, dst) in enumerate(fetches):
        pltpu.make_async_copy(src, dst, table_sem.at[n]).wait()
    in_tile = one_hot(iota((64, NPAIR), 1) // 16 == iota((64, NPAIR), 0))
    corners = 4.0 * dot(tile_ref[...].astype(f32).astype(bf16), in_tile)
    p_row = iota((1, NPAIR), 1)
    target = corners[0:1, :] + (p_row // 4 % 4).astype(f32)
    source = corners[1:2, :] + (p_row % 4).astype(f32)
    half = (iota((256, NPAIR), 0) // 2).astype(f32)
    hot_i = one_hot(half == target)
    hot_j = one_hot(half == source)
    orb_row = iota((NORB, NPAIR), 0).astype(f32)
    mask_of = dot(mask_ref[...].astype(f32).astype(bf16), one_hot(orb_row == source))
    live = jnp.sum(jnp.where(orb_row == target, mask_of, 0.0), axis=0, keepdims=True)
    before = one_hot(iota((LANES, LANES), 0) < iota((LANES, LANES), 1))
    every = jnp.ones((LANES, LANES), bf16)
    running = jnp.zeros((8, LANES), f32)
    ranks = []
    for n in range(NPAIR // LANES):
        flags = jnp.broadcast_to(live[:, n * LANES : (n + 1) * LANES], (8, LANES))
        bits = flags.astype(bf16)
        rank = dot(bits, before) + running
        running = running + dot(bits, every)
        ranks.append(jnp.where(flags > 0.5, rank, -1.0)[0:1, :])
    rank = jnp.concatenate(ranks, axis=1)

    same_plane = iota((PREP, 256), 0) % 2 == iota((PREP, 256), 1) % 2

    def select_rows(r, carry):
        rows = pl.ds(pl.multiple_of(r * PREP, PREP), PREP)
        slot = ((iota((PREP, NPAIR), 0) + r * PREP) // 2).astype(f32)
        chosen = one_hot(slot == rank)
        sel_i[rows, :] = jnp.where(same_plane, dot_nt(chosen, hot_i), 0.0).astype(bf16)
        sel_j[rows, :] = jnp.where(same_plane, dot_nt(chosen, hot_j), 0.0).astype(bf16)
        sel_t[r] = jnp.where(same_plane, dot_nt(hot_i, chosen), 0.0).astype(bf16)
        return carry

    lax.fori_loop(0, ROWS // PREP, select_rows, 0)

    widen = one_hot(iota((256, NORB), 0) // 2 == iota((256, NORB), 1))
    widen_t = one_hot(iota((NORB, 256), 0) == iota((NORB, 256), 1) // 2)
    for n, part in enumerate(split(rotation_ref[...])):
        tall = dot_nt(widen, part).astype(bf16)
        rot_k[n] = jnp.where(same_plane, dot(tall, widen_t), 0.0).astype(bf16)

    def fill_green(n, carry):
        green[n] = coupling / (syz_ref[...] + sx_ref[pl.ds(n, 1), :])
        return carry

    lax.fori_loop(0, NX // 2, fill_green, 0)

    arrived(got, e1_r)

    got_h, got_l = split(got[...].reshape(256, LANES))
    rotated = dot(rot_k[0], got_h) + dot(rot_k[0], got_l) + dot(rot_k[1], got_h)
    rotated = jnp.concatenate(split(rotated), axis=1)

    def density_rows(r, carry):
        rows = pl.ds(pl.multiple_of(r * 128, 128), 128)
        wide_i = dot(sel_i[rows, :], rotated)
        wide_j = dot(sel_j[rows, :], rotated)
        at_j = wide_j[:, :LANES] + wide_j[:, LANES:]
        rot_j[rows, :] = at_j
        density = (wide_i[:, :LANES] + wide_i[:, LANES:]) * at_j
        spectrum = z_product(density, tz_ref[...])
        dens[pl.ds(r * 4, 4)] = spectrum.reshape(4, 32, LANES)
        return carry

    lax.fori_loop(0, ROWS // 128, density_rows, 0)

    ours = pl.ds(2 * g, 2)

    def z_rows(z2):
        return pl.ds(2 * z2, 2)

    def z_rows_b(z2):
        return pl.ds(16 + 2 * z2, 2)

    for j in range(XDIM):

        @pl.loop(0, peers(j))
        def _(i):
            o2 = ahead(j, i)
            to_orb(dens.at[o2, pl.ds(0, 16), :], ra.at[j * YDIM + i], a1_s, a1_r.at[j], o2)

        @pl.loop(0, ZDIM - 1)
        def _(i):
            z2 = z_peer(i)
            to_grid(
                dens.at[block(j), z_rows_b(z2), :], rb.at[block(j), ours, :], b1_s, b1_r.at[j], 2 * z2 + 1
            )

        @pl.when(c == 1)
        def _():
            here(dens.at[block(j), z_rows_b(z), :], rb.at[block(j), ours, :], b1_r.at[j])

        @pl.when(c == 0)
        def _():
            to_grid(
                dens.at[block(j), z_rows_b(z), :], rb.at[block(j), ours, :], b1_s, b1_r.at[j], 2 * z + 1
            )

    here(dens.at[o, pl.ds(0, 16), :], ra.at[N_ORB - 1], a1_r.at[XDIM - 1])

    for j in range(XDIM):
        arrived(ra.at[chunk(j)], a1_r.at[j])

        @pl.loop(0, ZDIM - 1)
        def _(i):
            z2 = z_peer(i)
            to_grid(ra.at[chunk(j), z_rows(z2), :], box.at[chunk(j), ours, :], a2_s, x_ra.at[j], 2 * z2)

        @pl.when(c == 0)
        def _():
            here(ra.at[chunk(j), z_rows(z), :], box.at[chunk(j), ours, :], x_ra.at[j])

        @pl.when(c == 1)
        def _():
            to_grid(ra.at[chunk(j), z_rows(z), :], box.at[chunk(j), ours, :], a2_s, x_ra.at[j], 2 * z)
            arrived(rb.at[block(j)], b1_r.at[j])

            @pl.loop(0, peers(j))
            def _(i):
                o2 = ahead(j, i)
                to_orb(rb.at[o2], box.at[j * YDIM + i], b2_s, x_rb.at[j], o2)

            if DX[j] == 0:
                here(rb.at[o], box.at[N_ORB - 1], x_rb.at[j])

    for j in range(XDIM):

        @pl.when(c == 0)
        def _():
            arrived(box.at[chunk(j)], x_ra.at[j])

        @pl.when(c == 1)
        def _():
            arrived(box.at[chunk(j)], x_rb.at[j])

        for h in range(2):
            places = [j * YDIM + h * 4 + n for n in range(4)]
            v = jnp.concatenate([box[p] for p in places], axis=1)
            high, low = split(v)
            w = dot(tx_ref[...], jnp.concatenate([high, low, high], axis=0))
            for n in range(4):
                start = pl.multiple_of(behind(j, h * 4 + n) * NX, NX)
                mid[pl.ds(start, NX), :] = w[:, n * LANES : (n + 1) * LANES]

    low_half = iota((N_ORB, LANES), 1) < NZ

    for n in range(NX // 2):
        v0 = mid[pl.ds(2 * n, N_ORB, stride=NX), :]
        v1 = mid[pl.ds(2 * n + 1, N_ORB, stride=NX), :]
        even = jnp.where(low_half, v0, pltpu.roll(v1, NZ, 1))
        odd = jnp.where(low_half, pltpu.roll(v0, NZ, 1), v1)
        high, low = split(jnp.concatenate([even, odd], axis=0))
        spectrum = dot(tyf_ref[...], jnp.concatenate([high, low, high], axis=0)) * green[n]
        high, low = split(spectrum)
        w = dot(tyi_ref[...], jnp.concatenate([high, low, high], axis=0))
        even, odd = w[:N_ORB], w[N_ORB:]
        mid[pl.ds(2 * n, N_ORB, stride=NX), :] = jnp.where(low_half, even, pltpu.roll(odd, NZ, 1))
        mid[pl.ds(2 * n + 1, N_ORB, stride=NX), :] = jnp.where(low_half, pltpu.roll(even, NZ, 1), odd)

    for j in range(XDIM):
        for h in range(2):
            starts = [pl.multiple_of(behind(j, h * 4 + n) * NX, NX) for n in range(4)]
            v = jnp.concatenate([mid[pl.ds(s, NX), :] for s in starts], axis=1)
            high, low = split(v)
            w = dot(tx_ref[...], jnp.concatenate([high, low, high], axis=0))
            for n in range(4):
                pot[j * YDIM + h * 4 + n] = w[:, n * LANES : (n + 1) * LANES]

        @pl.when(c == 0)
        def _():
            @pl.loop(0, 2 * (ZDIM - 1))
            def _(i):
                g2 = 2 * z_peer(i // 2) + i % 2
                to_grid(
                    pot.at[chunk(j), pl.ds(2 * g2, 2), :], ra2.at[chunk(j), z_rows(z), :],
                    c1_s, c1_r.at[j], g2,
                )

            to_grid(
                pot.at[chunk(j), pl.ds(2 * (2 * z + 1), 2), :], ra2.at[chunk(j), z_rows(z), :],
                c1_s, c1_r.at[j], 2 * z + 1,
            )
            here(pot.at[chunk(j), ours, :], ra2.at[chunk(j), z_rows(z), :], c1_r.at[j])

        @pl.when(c == 1)
        def _():
            @pl.loop(0, peers(j))
            def _(i):
                to_orb(pot.at[j * YDIM + i], rb2.at[o], d1_s, d1_r.at[j], behind(j, i))

            if DX[j] == 0:
                here(pot.at[N_ORB - 1], rb2.at[o], d1_r.at[j])

    for j in range(XDIM):
        arrived(ra2.at[chunk(j)], c1_r.at[j])

        @pl.loop(0, peers(j))
        def _(i):
            to_orb(
                ra2.at[j * YDIM + i], back.at[o, pl.ds(0, 16), :], c2_s, c2_r.at[j], behind(j, i)
            )

        if DX[j] == 0:
            here(ra2.at[N_ORB - 1], back.at[o, pl.ds(0, 16), :], c2_r.at[j])

        @pl.when(c == 1)
        def _():
            arrived(rb2.at[block(j)], d1_r.at[j])

            @pl.loop(0, 2 * (ZDIM - 1))
            def _(i):
                g2 = 2 * z_peer(i // 2) + i % 2
                to_grid(
                    rb2.at[block(j), pl.ds(2 * g2, 2), :], back.at[block(j), z_rows_b(z), :],
                    d2_s, d2_r.at[j], g2,
                )

            to_grid(
                rb2.at[block(j), pl.ds(2 * (2 * z), 2), :], back.at[block(j), z_rows_b(z), :],
                d2_s, d2_r.at[j], 2 * z,
            )
            here(rb2.at[block(j), ours, :], back.at[block(j), z_rows_b(z), :], d2_r.at[j])

    total = jnp.zeros((256, 2 * LANES), f32)
    for j in range(XDIM):
        r = (x + DX[j]) % XDIM
        arrived(back.at[block(j), pl.ds(0, 16), :], c2_r.at[j])
        arrived(back.at[block(j), pl.ds(16, 16), :], d2_r.at[j])
        rows = pl.ds(pl.multiple_of(r * PREP, PREP), PREP)
        potential = z_product(back[block(j)].reshape(PREP, LANES), tz_ref[...])
        products = jnp.concatenate(split(potential * rot_j[rows, :]), axis=1)
        total = total + dot(sel_t[r], products)
    term[...] = (-(total[:, :LANES] + total[:, LANES:])).reshape(N_ORB, 8, LANES)

    for j in range(XDIM):

        @pl.loop(0, peers(j))
        def _(i):
            o2 = ahead(j, i)
            to_orb(term.at[o2], gathered.at[:, cells(o)], e4_s, e4_r, o2)

    here(term.at[o], gathered.at[:, cells(o)], e4_r)

    most = pl.ds(0, N_ORB - 1)
    arrived(got.at[most], e1_s)
    arrived(ra.at[most], a1_s)
    arrived(term.at[most], e4_s)
    arrived(ra2.at[most], c2_s)

    @pl.when(c == 0)
    def _():
        arrived(rb.at[:, pl.ds(0, 16), :], b1_s)
        arrived(ra.at[:, pl.ds(0, 14), :], a2_s)
        arrived(pot.at[:, pl.ds(0, 30), :], c1_s)

    @pl.when(c == 1)
    def _():
        arrived(rb.at[:, pl.ds(0, 14), :], b1_s)
        arrived(ra.at[:, pl.ds(0, 16), :], a2_s)
        arrived(rb.at[most], b2_s)
        arrived(pot.at[most], d1_s)
        arrived(rb2.at[:, pl.ds(0, 30), :], d2_s)

    arrived(gathered, e4_r)
    stores = [
        (gathered.at[pl.ds(2 * n, 2), :], out_ref.at[n], out_sem.at[n]) for n in range(4)
    ]
    for args in stores:
        pltpu.make_async_copy(*args).start()
    for args in stores:
        pltpu.make_async_copy(*args).wait()


def on_device(orbitals, rotation, tile_list, pair_mask):
    consts = [jnp.asarray(t) for t in tables()]
    anyspace = pl.BlockSpec(memory_space=pl.ANY)
    dma = pltpu.SemaphoreType.DMA
    box = pltpu.VMEM((N_ORB, NX, LANES), f32)
    half_box = pltpu.VMEM((N_ORB, 16, LANES), f32)
    operands = [rotation, tile_list.T, pair_mask, *consts]
    return pl.pallas_call(
        kernel,
        out_shape=jax.ShapeDtypeStruct(orbitals.shape, f32),
        in_specs=[anyspace] * (4 + len(consts)),
        out_specs=anyspace,
        scratch_shapes=[pltpu.VMEM(a.shape, a.dtype) for a in operands]
        + [
            pltpu.VMEM((8, NY * NZ), f32),
            pltpu.VMEM((N_ORB, 8, LANES), f32),
            pltpu.VMEM((ROWS, 256), bf16),
            pltpu.VMEM((ROWS, 256), bf16),
            pltpu.VMEM((ROWS // PREP, 256, PREP), bf16),
            pltpu.VMEM((2, 256, 256), bf16),
            pltpu.VMEM((ROWS, LANES), f32),
            pltpu.VMEM((NX // 2, NY, LANES), f32),
            box,
            half_box,
            box,
            box,
            pltpu.VMEM((N_ORB * NX, LANES), f32),
            box,
            half_box,
            box,
            box,
            pltpu.VMEM((N_ORB, 8, LANES), f32),
            pltpu.VMEM((8, NY * NZ), f32),
            dma((4,)),
            dma((4,)),
            dma((len(operands),)),
        ]
        + [dma((XDIM,))] * 8
        + [dma] * 12,
        compiler_params=pltpu.CompilerParams(
            collective_id=0, has_side_effects=True, vmem_limit_bytes=67_000_000
        ),
    )(orbitals, *operands)


def solution(mesh):
    in_specs = (P("orb", "grid", None), P(), P(), P())
    out_specs = P("orb", "grid", None)
    return jax.shard_map(
        on_device, mesh=mesh, in_specs=in_specs, out_specs=out_specs, check_vma=False
    )
```

```python
import numpy as np
import jax
import jax.numpy as jnp
from jax import lax
from jax.experimental import pallas as pl
from jax.experimental.pallas import tpu as pltpu
from jax.sharding import PartitionSpec as P

NORB = 128
NX = 32
NY = 64
NZ = 64
NPAIR = 1024
LANES = 128
N_ORB = 32
N_GRID = 16
XDIM = 4
YDIM = 8
ZDIM = 8
CHUNKS = 4
CHUNK = 8
PEERS = sorted(
    ((dx, dy) for dx in (2, 1, -1, 0) for dy in (4, 3, -3, 2, -2, 1, -1, 0)),
    key=lambda step: -abs(step[0]) - abs(step[1]),
)
Z_STEPS = (4, 3, -3, 2, -2, 1, -1)
ROWS = 1024
PREP = 256
coupling = 0.25
screening = 0.1
MESH = pl.DeviceIdType.MESH
f32 = jnp.float32
bf16 = jnp.bfloat16


def sine_table(length):
    k = np.arange(length, dtype=np.float64) + 1.0
    return np.sqrt(2.0 / (length + 1.0)) * np.sin(np.pi * k[:, None] * k[None, :] / (length + 1.0))


def eigen_values(length):
    k = np.arange(length, dtype=np.float64) + 1.0
    return 2.0 - 2.0 * np.cos(np.pi * k / (length + 1.0))


def halves(table):
    high = table.astype(np.float32).astype(jnp.bfloat16)
    low = (table - high.astype(np.float64)).astype(np.float32).astype(jnp.bfloat16)
    return high, low


def tables():
    sx_h, sx_l = halves(sine_table(NX))
    table_x = np.concatenate([sx_h, sx_h, sx_l], axis=1)
    s = sine_table(NY)
    split_cols = np.concatenate([s[:, 0::2], s[:, 1::2]], axis=1)
    fh, fl = halves(split_cols)
    table_yf = np.concatenate([fh, fh, fl], axis=1)
    ih, il = halves(split_cols.T)
    table_yi = np.concatenate([ih, ih, il], axis=1)
    block = np.kron(np.eye(2), sine_table(NZ))
    bh, bl = halves(block)
    table_z = np.concatenate([bh, bl], axis=1)
    ly, lz, lx = eigen_values(NY), eigen_values(NZ), eigen_values(NX)
    sum_yz = ly[:, None] + np.tile(lz, 2)[None, :] + screening
    sum_x = np.repeat(lx.reshape(NX // 2, 2), NZ, axis=1)
    return (
        table_x,
        table_yf,
        table_yi,
        table_z,
        sum_yz.astype(np.float32),
        sum_x.astype(np.float32),
    )


def split(v):
    high = v.astype(bf16)
    low = (v - high.astype(f32)).astype(bf16)
    return high, low


def dot(a, b):
    return jnp.dot(a, b, preferred_element_type=f32)


def dot_nt(a, b):
    return lax.dot_general(a, b, (((1,), (1,)), ((), ())), preferred_element_type=f32)


def iota(shape, dim):
    return lax.broadcasted_iota(jnp.int32, shape, dim)


def one_hot(cond):
    return jnp.where(cond, 1.0, 0.0).astype(bf16)


def z_product(v, table_z):
    high, low = split(v)
    a = dot(high, table_z)
    return a[:, :LANES] + a[:, LANES:] + dot(low, table_z[:, :LANES])


def kernel(
    orb_hbm, rotation_hbm, tile_hbm, mask_hbm, tx_hbm, tyf_hbm, tyi_hbm, tz_hbm, syz_hbm, sx_hbm,
    out_ref,
    rotation_ref, tile_ref, mask_ref, tx_ref, tyf_ref, tyi_ref, tz_ref, syz_ref, sx_ref,
    own, got, sel_i, sel_j, sel_t, rot_k, rot_j, green, dens,
    ra, rb, box, mid, pot, ra2, rb2, back, term, gathered,
    in_sem, out_sem, table_sem,
    a1_r, b1_r, x_ra, x_rb, c1_r, d1_r, c2_r, d2_r,
    e1_r, e4_r, e1_s, a1_s, b1_s, a2_s, b2_s, c1_s, d1_s, c2_s, d2_s, e4_s,
):
    o = lax.axis_index("orb")
    g = lax.axis_index("grid")
    x, y = o // YDIM, o % YDIM
    z, c = g // 2, g % 2

    def ahead(k):
        dx, dy = PEERS[k]
        return (x + dx % XDIM) % XDIM * YDIM + (y + dy % YDIM) % YDIM

    def behind(k):
        dx, dy = PEERS[k]
        return (x + -dx % XDIM) % XDIM * YDIM + (y + -dy % YDIM) % YDIM

    def chunk(j):
        return pl.ds(j * CHUNK, CHUNK)

    def members(j):
        return range(j * CHUNK, min((j + 1) * CHUNK, N_ORB - 1))

    others = range(N_ORB - 1)
    z_peers = [(z + step % ZDIM) % ZDIM for step in Z_STEPS]

    def to_orb(src, dst, s_sem, r_sem, o2):
        pltpu.make_async_remote_copy(
            src_ref=src, dst_ref=dst, send_sem=s_sem, recv_sem=r_sem,
            device_id=(o2, g), device_id_type=MESH,
        ).start()

    def to_grid(src, dst, s_sem, r_sem, g2):
        pltpu.make_async_remote_copy(
            src_ref=src, dst_ref=dst, send_sem=s_sem, recv_sem=r_sem,
            device_id=(o, g2), device_id_type=MESH,
        ).start()

    def here(src, dst, r_sem):
        pltpu.make_async_copy(src, dst, r_sem).start()

    def arrived(ref, sem):
        pltpu.make_async_copy(ref, ref, sem).wait()

    loads = [
        (orb_hbm.at[n], own.at[pl.ds(2 * n, 2), :], in_sem.at[n]) for n in range(4)
    ]
    fetches = [
        (tile_hbm, tile_ref), (mask_hbm, mask_ref), (rotation_hbm, rotation_ref),
        (syz_hbm, syz_ref), (sx_hbm, sx_ref), (tz_hbm, tz_ref),
        (tx_hbm, tx_ref), (tyf_hbm, tyf_ref), (tyi_hbm, tyi_ref),
    ]
    for args in loads:
        pltpu.make_async_copy(*args).start()
    for n, (src, dst) in enumerate(fetches):
        pltpu.make_async_copy(src, dst, table_sem.at[n]).start()
    barrier = pltpu.get_barrier_semaphore()
    for k in others:
        pl.semaphore_signal(barrier, inc=1, device_id=(ahead(k), g), device_id_type=MESH)
    for z2 in z_peers:
        for core in range(2):
            pl.semaphore_signal(barrier, inc=1, device_id=(o, 2 * z2 + core), device_id_type=MESH)
    pl.semaphore_signal(barrier, inc=1, device_id=(o, 2 * z + 1 - c), device_id_type=MESH)
    for args in loads:
        pltpu.make_async_copy(*args).wait()
    pl.semaphore_wait(barrier, N_ORB - 1 + N_GRID - 1)

    def cells(o2):
        return pl.ds(pl.multiple_of(o2 * LANES, LANES), LANES)

    for k in others:
        to_orb(own.at[:, cells(ahead(k))], got.at[o], e1_s, e1_r, ahead(k))
    here(own.at[:, cells(o)], got.at[o], e1_r)

    for n, (src, dst) in enumerate(fetches):
        pltpu.make_async_copy(src, dst, table_sem.at[n]).wait()
    in_tile = one_hot(iota((64, NPAIR), 1) // 16 == iota((64, NPAIR), 0))
    corners = 4.0 * dot(tile_ref[...].astype(f32).astype(bf16), in_tile)
    p_row = iota((1, NPAIR), 1)
    target = corners[0:1, :] + (p_row // 4 % 4).astype(f32)
    source = corners[1:2, :] + (p_row % 4).astype(f32)
    half = (iota((256, NPAIR), 0) // 2).astype(f32)
    hot_i = one_hot(half == target)
    hot_j = one_hot(half == source)
    orb_row = iota((NORB, NPAIR), 0).astype(f32)
    mask_of = dot(mask_ref[...].astype(f32).astype(bf16), one_hot(orb_row == source))
    live = jnp.sum(jnp.where(orb_row == target, mask_of, 0.0), axis=0, keepdims=True)
    before = one_hot(iota((LANES, LANES), 0) < iota((LANES, LANES), 1))
    every = jnp.ones((LANES, LANES), bf16)
    running = jnp.zeros((8, LANES), f32)
    ranks = []
    for n in range(NPAIR // LANES):
        flags = jnp.broadcast_to(live[:, n * LANES : (n + 1) * LANES], (8, LANES))
        bits = flags.astype(bf16)
        rank = dot(bits, before) + running
        running = running + dot(bits, every)
        ranks.append(jnp.where(flags > 0.5, rank, -1.0)[0:1, :])
    rank = jnp.concatenate(ranks, axis=1)

    same_plane = iota((PREP, 256), 0) % 2 == iota((PREP, 256), 1) % 2

    slot = (iota((32, NPAIR), 0) // 2).astype(f32)
    for j in range(CHUNKS):
        rows = pl.ds(j * PREP, PREP)
        parts = [
            one_hot(slot == rank - (16 * ahead(k)).astype(f32))
            for k in range(j * CHUNK, (j + 1) * CHUNK)
        ]
        chosen = jnp.concatenate(parts, axis=0)
        sel_i[rows, :] = jnp.where(same_plane, dot_nt(chosen, hot_i), 0.0).astype(bf16)
        sel_j[rows, :] = jnp.where(same_plane, dot_nt(chosen, hot_j), 0.0).astype(bf16)
        sel_t[j] = jnp.where(same_plane, dot_nt(hot_i, chosen), 0.0).astype(bf16)

    widen = one_hot(iota((256, NORB), 0) // 2 == iota((256, NORB), 1))
    widen_t = one_hot(iota((NORB, 256), 0) == iota((NORB, 256), 1) // 2)
    for n, part in enumerate(split(rotation_ref[...])):
        tall = dot_nt(widen, part).astype(bf16)
        rot_k[n] = jnp.where(same_plane, dot(tall, widen_t), 0.0).astype(bf16)

    def fill_green(n, carry):
        green[n] = coupling / (syz_ref[...] + sx_ref[pl.ds(n, 1), :])
        return carry

    lax.fori_loop(0, NX // 2, fill_green, 0)

    arrived(got, e1_r)

    got_h, got_l = split(got[...].reshape(256, LANES))
    rotated = dot(rot_k[0], got_h) + dot(rot_k[0], got_l) + dot(rot_k[1], got_h)
    rotated = jnp.concatenate(split(rotated), axis=1)

    def density_rows(j):
        for h in range(2):
            rows = pl.ds(j * PREP + h * 128, 128)
            wide_i = dot(sel_i[rows, :], rotated)
            wide_j = dot(sel_j[rows, :], rotated)
            at_j = wide_j[:, :LANES] + wide_j[:, LANES:]
            rot_j[rows, :] = at_j
            density = (wide_i[:, :LANES] + wide_i[:, LANES:]) * at_j
            spectrum = z_product(density, tz_ref[...])
            dens[pl.ds(j * CHUNK + h * 4, 4)] = spectrum.reshape(4, 32, LANES)

    ours = pl.ds(2 * g, 2)

    def z_rows(z2):
        return pl.ds(2 * z2, 2)

    def z_rows_b(z2):
        return pl.ds(16 + 2 * z2, 2)

    last = N_ORB - 1
    for j in range(CHUNKS):
        density_rows(j)
        for k in members(j):
            to_orb(dens.at[k, pl.ds(0, 16), :], ra.at[k], a1_s, a1_r.at[j], ahead(k))
        for z2 in z_peers:
            to_grid(
                dens.at[chunk(j), z_rows_b(z2), :], rb.at[chunk(j), ours, :], b1_s, b1_r.at[j], 2 * z2 + 1
            )

        @pl.when(c == 1)
        def _():
            here(dens.at[chunk(j), z_rows_b(z), :], rb.at[chunk(j), ours, :], b1_r.at[j])

        @pl.when(c == 0)
        def _():
            to_grid(
                dens.at[chunk(j), z_rows_b(z), :], rb.at[chunk(j), ours, :], b1_s, b1_r.at[j], 2 * z + 1
            )

    here(dens.at[last, pl.ds(0, 16), :], ra.at[last], a1_r.at[CHUNKS - 1])

    for j in range(CHUNKS):
        arrived(ra.at[chunk(j)], a1_r.at[j])
        for z2 in z_peers:
            to_grid(ra.at[chunk(j), z_rows(z2), :], box.at[chunk(j), ours, :], a2_s, x_ra.at[j], 2 * z2)

        @pl.when(c == 0)
        def _():
            here(ra.at[chunk(j), z_rows(z), :], box.at[chunk(j), ours, :], x_ra.at[j])

        @pl.when(c == 1)
        def _():
            to_grid(ra.at[chunk(j), z_rows(z), :], box.at[chunk(j), ours, :], a2_s, x_ra.at[j], 2 * z)
            arrived(rb.at[chunk(j)], b1_r.at[j])
            for k in members(j):
                to_orb(rb.at[k], box.at[k], b2_s, x_rb.at[j], ahead(k))
            if j == CHUNKS - 1:
                here(rb.at[last], box.at[last], x_rb.at[j])

    for j in range(CHUNKS):

        @pl.when(c == 0)
        def _():
            arrived(box.at[chunk(j)], x_ra.at[j])

        @pl.when(c == 1)
        def _():
            arrived(box.at[chunk(j)], x_rb.at[j])

        for h in range(2):
            places = [j * CHUNK + h * 4 + n for n in range(4)]
            v = jnp.concatenate([box[k] for k in places], axis=1)
            high, low = split(v)
            w = dot(tx_ref[...], jnp.concatenate([high, low, high], axis=0))
            for n, k in enumerate(places):
                start = pl.multiple_of(behind(k) * NX, NX)
                mid[pl.ds(start, NX), :] = w[:, n * LANES : (n + 1) * LANES]

    low_half = iota((N_ORB, LANES), 1) < NZ

    for n in range(NX // 2):
        v0 = mid[pl.ds(2 * n, N_ORB, stride=NX), :]
        v1 = mid[pl.ds(2 * n + 1, N_ORB, stride=NX), :]
        even = jnp.where(low_half, v0, pltpu.roll(v1, NZ, 1))
        odd = jnp.where(low_half, pltpu.roll(v0, NZ, 1), v1)
        high, low = split(jnp.concatenate([even, odd], axis=0))
        spectrum = dot(tyf_ref[...], jnp.concatenate([high, low, high], axis=0)) * green[n]
        high, low = split(spectrum)
        w = dot(tyi_ref[...], jnp.concatenate([high, low, high], axis=0))
        even, odd = w[:N_ORB], w[N_ORB:]
        mid[pl.ds(2 * n, N_ORB, stride=NX), :] = jnp.where(low_half, even, pltpu.roll(odd, NZ, 1))
        mid[pl.ds(2 * n + 1, N_ORB, stride=NX), :] = jnp.where(low_half, pltpu.roll(even, NZ, 1), odd)

    for j in range(CHUNKS):
        for h in range(2):
            places = [j * CHUNK + h * 4 + n for n in range(4)]
            v = jnp.concatenate(
                [mid[pl.ds(pl.multiple_of(behind(k) * NX, NX), NX), :] for k in places], axis=1
            )
            high, low = split(v)
            w = dot(tx_ref[...], jnp.concatenate([high, low, high], axis=0))
            for n, k in enumerate(places):
                pot[k] = w[:, n * LANES : (n + 1) * LANES]

        @pl.when(c == 0)
        def _():
            for z2 in z_peers:
                for core in range(2):
                    g2 = 2 * z2 + core
                    to_grid(
                        pot.at[chunk(j), pl.ds(2 * g2, 2), :], ra2.at[chunk(j), z_rows(z), :],
                        c1_s, c1_r.at[j], g2,
                    )
            to_grid(
                pot.at[chunk(j), pl.ds(2 * (2 * z + 1), 2), :], ra2.at[chunk(j), z_rows(z), :],
                c1_s, c1_r.at[j], 2 * z + 1,
            )
            here(pot.at[chunk(j), ours, :], ra2.at[chunk(j), z_rows(z), :], c1_r.at[j])

        @pl.when(c == 1)
        def _():
            for k in members(j):
                to_orb(pot.at[k], rb2.at[k], d1_s, d1_r.at[j], behind(k))
            if j == CHUNKS - 1:
                here(pot.at[last], rb2.at[last], d1_r.at[j])

    for j in range(CHUNKS):
        arrived(ra2.at[chunk(j)], c1_r.at[j])
        for k in members(j):
            to_orb(ra2.at[k], back.at[k, pl.ds(0, 16), :], c2_s, c2_r.at[j], behind(k))
        if j == CHUNKS - 1:
            here(ra2.at[last], back.at[last, pl.ds(0, 16), :], c2_r.at[j])

        @pl.when(c == 1)
        def _():
            arrived(rb2.at[chunk(j)], d1_r.at[j])
            for z2 in z_peers:
                for core in range(2):
                    g2 = 2 * z2 + core
                    to_grid(
                        rb2.at[chunk(j), pl.ds(2 * g2, 2), :], back.at[chunk(j), z_rows_b(z), :],
                        d2_s, d2_r.at[j], g2,
                    )
            to_grid(
                rb2.at[chunk(j), pl.ds(2 * (2 * z), 2), :], back.at[chunk(j), z_rows_b(z), :],
                d2_s, d2_r.at[j], 2 * z,
            )
            here(rb2.at[chunk(j), ours, :], back.at[chunk(j), z_rows_b(z), :], d2_r.at[j])

    total = jnp.zeros((256, 2 * LANES), f32)
    for j in range(CHUNKS):
        arrived(back.at[chunk(j), pl.ds(0, 16), :], c2_r.at[j])
        arrived(back.at[chunk(j), pl.ds(16, 16), :], d2_r.at[j])
        rows = pl.ds(j * PREP, PREP)
        potential = z_product(back[chunk(j)].reshape(PREP, LANES), tz_ref[...])
        products = jnp.concatenate(split(potential * rot_j[rows, :]), axis=1)
        total = total + dot(sel_t[j], products)
    term[...] = (-(total[:, :LANES] + total[:, LANES:])).reshape(N_ORB, 8, LANES)

    for k in others:
        to_orb(term.at[ahead(k)], gathered.at[:, cells(o)], e4_s, e4_r, ahead(k))
    here(term.at[o], gathered.at[:, cells(o)], e4_r)

    most = pl.ds(0, N_ORB - 1)
    arrived(got.at[most], e1_s)
    arrived(ra.at[most], a1_s)
    arrived(term.at[most], e4_s)
    arrived(ra2.at[most], c2_s)

    @pl.when(c == 0)
    def _():
        arrived(rb.at[:, pl.ds(0, 16), :], b1_s)
        arrived(ra.at[:, pl.ds(0, 14), :], a2_s)
        arrived(pot.at[:, pl.ds(0, 30), :], c1_s)

    @pl.when(c == 1)
    def _():
        arrived(rb.at[:, pl.ds(0, 14), :], b1_s)
        arrived(ra.at[:, pl.ds(0, 16), :], a2_s)
        arrived(rb.at[most], b2_s)
        arrived(pot.at[most], d1_s)
        arrived(rb2.at[:, pl.ds(0, 30), :], d2_s)

    arrived(gathered, e4_r)
    stores = [
        (gathered.at[pl.ds(2 * n, 2), :], out_ref.at[n], out_sem.at[n]) for n in range(4)
    ]
    for args in stores:
        pltpu.make_async_copy(*args).start()
    for args in stores:
        pltpu.make_async_copy(*args).wait()


def on_device(orbitals, rotation, tile_list, pair_mask):
    consts = [jnp.asarray(t) for t in tables()]
    anyspace = pl.BlockSpec(memory_space=pl.ANY)
    dma = pltpu.SemaphoreType.DMA
    box = pltpu.VMEM((N_ORB, NX, LANES), f32)
    half_box = pltpu.VMEM((N_ORB, 16, LANES), f32)
    operands = [rotation, tile_list.T, pair_mask, *consts]
    return pl.pallas_call(
        kernel,
        out_shape=jax.ShapeDtypeStruct(orbitals.shape, f32),
        in_specs=[anyspace] * (4 + len(consts)),
        out_specs=anyspace,
        scratch_shapes=[pltpu.VMEM(a.shape, a.dtype) for a in operands]
        + [
            pltpu.VMEM((8, NY * NZ), f32),
            pltpu.VMEM((N_ORB, 8, LANES), f32),
            pltpu.VMEM((ROWS, 256), bf16),
            pltpu.VMEM((ROWS, 256), bf16),
            pltpu.VMEM((ROWS // PREP, 256, PREP), bf16),
            pltpu.VMEM((2, 256, 256), bf16),
            pltpu.VMEM((ROWS, LANES), f32),
            pltpu.VMEM((NX // 2, NY, LANES), f32),
            box,
            half_box,
            box,
            box,
            pltpu.VMEM((N_ORB * NX, LANES), f32),
            box,
            half_box,
            box,
            box,
            pltpu.VMEM((N_ORB, 8, LANES), f32),
            pltpu.VMEM((8, NY * NZ), f32),
            dma((4,)),
            dma((4,)),
            dma((len(operands),)),
        ]
        + [dma((CHUNKS,))] * 8
        + [dma] * 12,
        compiler_params=pltpu.CompilerParams(
            collective_id=0, has_side_effects=True, vmem_limit_bytes=67_000_000
        ),
    )(orbitals, *operands)


def solution(mesh):
    in_specs = (P("orb", "grid", None), P(), P(), P())
    out_specs = P("orb", "grid", None)
    return jax.shard_map(
        on_device, mesh=mesh, in_specs=in_specs, out_specs=out_specs, check_vma=False
    )
```

```python
import numpy as np
import jax
import jax.numpy as jnp
from jax import lax
from jax.experimental import pallas as pl
from jax.experimental.pallas import tpu as pltpu
from jax.sharding import PartitionSpec as P

NORB = 128
NX = 32
NY = 64
NZ = 64
NPAIR = 1024
LANES = 128
N_ORB = 32
N_GRID = 16
XDIM = 4
YDIM = 8
ZDIM = 8
CHUNKS = 4
CHUNK = 8
PEERS = sorted(
    ((dx, dy) for dx in (2, 1, -1, 0) for dy in (4, 3, -3, 2, -2, 1, -1, 0)),
    key=lambda step: -abs(step[0]) - abs(step[1]),
)
Z_STEPS = (4, 3, -3, 2, -2, 1, -1)
ROWS = 1024
PREP = 256
coupling = 0.25
screening = 0.1
MESH = pl.DeviceIdType.MESH
f32 = jnp.float32
bf16 = jnp.bfloat16


def sine_table(length):
    k = np.arange(length, dtype=np.float64) + 1.0
    return np.sqrt(2.0 / (length + 1.0)) * np.sin(np.pi * k[:, None] * k[None, :] / (length + 1.0))


def eigen_values(length):
    k = np.arange(length, dtype=np.float64) + 1.0
    return 2.0 - 2.0 * np.cos(np.pi * k / (length + 1.0))


def halves(table):
    high = table.astype(np.float32).astype(jnp.bfloat16)
    low = (table - high.astype(np.float64)).astype(np.float32).astype(jnp.bfloat16)
    return high, low


def tables():
    sx_h, sx_l = halves(sine_table(NX))
    table_x = np.concatenate([sx_h, sx_h, sx_l], axis=1)
    s = sine_table(NY)
    split_cols = np.concatenate([s[:, 0::2], s[:, 1::2]], axis=1)
    fh, fl = halves(split_cols)
    table_yf = np.concatenate([fh, fh, fl], axis=1)
    ih, il = halves(split_cols.T)
    table_yi = np.concatenate([ih, ih, il], axis=1)
    block = np.kron(np.eye(2), sine_table(NZ))
    bh, bl = halves(block)
    table_z = np.concatenate([bh, bl], axis=1)
    ly, lz, lx = eigen_values(NY), eigen_values(NZ), eigen_values(NX)
    sum_yz = ly[:, None] + np.tile(lz, 2)[None, :] + screening
    sum_x = np.repeat(lx.reshape(NX // 2, 2), NZ, axis=1)
    return (
        table_x,
        table_yf,
        table_yi,
        table_z,
        sum_yz.astype(np.float32),
        sum_x.astype(np.float32),
    )


def split(v):
    high = v.astype(bf16)
    low = (v - high.astype(f32)).astype(bf16)
    return high, low


def dot(a, b):
    return jnp.dot(a, b, preferred_element_type=f32)


def dot_nt(a, b):
    return lax.dot_general(a, b, (((1,), (1,)), ((), ())), preferred_element_type=f32)


def iota(shape, dim):
    return lax.broadcasted_iota(jnp.int32, shape, dim)


def one_hot(cond):
    return jnp.where(cond, 1.0, 0.0).astype(bf16)


def z_product(v, table_z):
    high, low = split(v)
    a = dot(high, table_z)
    return a[:, :LANES] + a[:, LANES:] + dot(low, table_z[:, :LANES])


def kernel(
    orb_hbm, rotation_hbm, tile_hbm, mask_hbm, tx_hbm, tyf_hbm, tyi_hbm, tz_hbm, syz_hbm, sx_hbm,
    out_ref,
    rotation_ref, tile_ref, mask_ref, tx_ref, tyf_ref, tyi_ref, tz_ref, syz_ref, sx_ref,
    own, got, sel_i, sel_j, sel_t, rot_k, rot_j, green, dens,
    ra, rb, box, mid, pot, ra2, rb2, back, term, gathered,
    in_sem, out_sem, table_sem,
    a1_r, b1_r, x_ra, x_rb, c1_r, d1_r, c2_r, d2_r,
    e1_r, e4_r, e1_s, a1_s, b1_s, a2_s, b2_s, c1_s, d1_s, c2_s, d2_s, e4_s,
):
    o = lax.axis_index("orb")
    g = lax.axis_index("grid")
    x, y = o // YDIM, o % YDIM
    z, c = g // 2, g % 2

    def ahead(k):
        dx, dy = PEERS[k]
        return (x + dx % XDIM) % XDIM * YDIM + (y + dy % YDIM) % YDIM

    def behind(k):
        dx, dy = PEERS[k]
        return (x + -dx % XDIM) % XDIM * YDIM + (y + -dy % YDIM) % YDIM

    def chunk(j):
        return pl.ds(j * CHUNK, CHUNK)

    def members(j):
        return range(j * CHUNK, min((j + 1) * CHUNK, N_ORB - 1))

    others = range(N_ORB - 1)
    z_peers = [(z + step % ZDIM) % ZDIM for step in Z_STEPS]

    def to_orb(src, dst, s_sem, r_sem, o2):
        pltpu.make_async_remote_copy(
            src_ref=src, dst_ref=dst, send_sem=s_sem, recv_sem=r_sem,
            device_id=(o2, g), device_id_type=MESH,
        ).start()

    def to_grid(src, dst, s_sem, r_sem, g2):
        pltpu.make_async_remote_copy(
            src_ref=src, dst_ref=dst, send_sem=s_sem, recv_sem=r_sem,
            device_id=(o, g2), device_id_type=MESH,
        ).start()

    def here(src, dst, r_sem):
        pltpu.make_async_copy(src, dst, r_sem).start()

    def arrived(ref, sem):
        pltpu.make_async_copy(ref, ref, sem).wait()

    loads = [
        (orb_hbm.at[n], own.at[pl.ds(2 * n, 2), :], in_sem.at[n]) for n in range(4)
    ]
    fetches = [
        (tile_hbm, tile_ref), (mask_hbm, mask_ref), (rotation_hbm, rotation_ref),
        (syz_hbm, syz_ref), (sx_hbm, sx_ref), (tz_hbm, tz_ref),
        (tx_hbm, tx_ref), (tyf_hbm, tyf_ref), (tyi_hbm, tyi_ref),
    ]
    barrier = pltpu.get_barrier_semaphore()
    for k in others:
        pl.semaphore_signal(barrier, inc=1, device_id=(ahead(k), g), device_id_type=MESH)
    for z2 in z_peers:
        for core in range(2):
            pl.semaphore_signal(barrier, inc=1, device_id=(o, 2 * z2 + core), device_id_type=MESH)
    pl.semaphore_signal(barrier, inc=1, device_id=(o, 2 * z + 1 - c), device_id_type=MESH)
    for args in loads:
        pltpu.make_async_copy(*args).start()
    for n, (src, dst) in enumerate(fetches):
        pltpu.make_async_copy(src, dst, table_sem.at[n]).start()
    for args in loads:
        pltpu.make_async_copy(*args).wait()
    pl.semaphore_wait(barrier, N_ORB - 1 + N_GRID - 1)

    def cells(o2):
        return pl.ds(pl.multiple_of(o2 * LANES, LANES), LANES)

    for k in others:
        to_orb(own.at[:, cells(ahead(k))], got.at[o], e1_s, e1_r, ahead(k))
    here(own.at[:, cells(o)], got.at[o], e1_r)

    for n, (src, dst) in enumerate(fetches):
        pltpu.make_async_copy(src, dst, table_sem.at[n]).wait()
    in_tile = one_hot(iota((64, NPAIR), 1) // 16 == iota((64, NPAIR), 0))
    corners = 4.0 * dot(tile_ref[...].astype(f32).astype(bf16), in_tile)
    p_row = iota((1, NPAIR), 1)
    target = corners[0:1, :] + (p_row // 4 % 4).astype(f32)
    source = corners[1:2, :] + (p_row % 4).astype(f32)
    half = (iota((256, NPAIR), 0) // 2).astype(f32)
    hot_i = one_hot(half == target)
    hot_j = one_hot(half == source)
    orb_row = iota((NORB, NPAIR), 0).astype(f32)
    mask_of = dot(mask_ref[...].astype(f32).astype(bf16), one_hot(orb_row == source))
    live = jnp.sum(jnp.where(orb_row == target, mask_of, 0.0), axis=0, keepdims=True)
    before = one_hot(iota((LANES, LANES), 0) < iota((LANES, LANES), 1))
    every = jnp.ones((LANES, LANES), bf16)
    running = jnp.zeros((8, LANES), f32)
    ranks = []
    for n in range(NPAIR // LANES):
        flags = jnp.broadcast_to(live[:, n * LANES : (n + 1) * LANES], (8, LANES))
        bits = flags.astype(bf16)
        rank = dot(bits, before) + running
        running = running + dot(bits, every)
        ranks.append(jnp.where(flags > 0.5, rank, -1.0)[0:1, :])
    rank = jnp.concatenate(ranks, axis=1)

    same_plane = iota((PREP, 256), 0) % 2 == iota((PREP, 256), 1) % 2

    slot = (iota((32, NPAIR), 0) // 2).astype(f32)
    for j in range(CHUNKS):
        rows = pl.ds(j * PREP, PREP)
        parts = [
            one_hot(slot == rank - (16 * ahead(k)).astype(f32))
            for k in range(j * CHUNK, (j + 1) * CHUNK)
        ]
        chosen = jnp.concatenate(parts, axis=0)
        sel_i[rows, :] = jnp.where(same_plane, dot_nt(chosen, hot_i), 0.0).astype(bf16)
        sel_j[rows, :] = jnp.where(same_plane, dot_nt(chosen, hot_j), 0.0).astype(bf16)
        sel_t[j] = jnp.where(same_plane, dot_nt(hot_i, chosen), 0.0).astype(bf16)

    widen = one_hot(iota((256, NORB), 0) // 2 == iota((256, NORB), 1))
    widen_t = one_hot(iota((NORB, 256), 0) == iota((NORB, 256), 1) // 2)
    for n, part in enumerate(split(rotation_ref[...])):
        tall = dot_nt(widen, part).astype(bf16)
        rot_k[n] = jnp.where(same_plane, dot(tall, widen_t), 0.0).astype(bf16)

    def fill_green(n, carry):
        green[n] = coupling / (syz_ref[...] + sx_ref[pl.ds(n, 1), :])
        return carry

    lax.fori_loop(0, NX // 2, fill_green, 0)

    arrived(got, e1_r)

    got_h, got_l = split(got[...].reshape(256, LANES))
    rotated = dot(rot_k[0], got_h) + dot(rot_k[0], got_l) + dot(rot_k[1], got_h)
    rotated = jnp.concatenate(split(rotated), axis=1)

    def density_rows(j, h):
        rows = pl.ds(j * PREP + h * 128, 128)
        wide_i = dot(sel_i[rows, :], rotated)
        wide_j = dot(sel_j[rows, :], rotated)
        at_j = wide_j[:, :LANES] + wide_j[:, LANES:]
        rot_j[rows, :] = at_j
        density = (wide_i[:, :LANES] + wide_i[:, LANES:]) * at_j
        spectrum = z_product(density, tz_ref[...])
        dens[pl.ds(j * CHUNK + h * 4, 4)] = spectrum.reshape(4, 32, LANES)

    ours = pl.ds(2 * g, 2)

    def z_rows(z2):
        return pl.ds(2 * z2, 2)

    def z_rows_b(z2):
        return pl.ds(16 + 2 * z2, 2)

    last = N_ORB - 1
    for j in range(CHUNKS):
        for h in range(2):
            density_rows(j, h)
            for k in members(j)[h * 4 : h * 4 + 4]:
                to_orb(dens.at[k, pl.ds(0, 16), :], ra.at[k], a1_s, a1_r.at[j], ahead(k))
        for z2 in z_peers:
            to_grid(
                dens.at[chunk(j), z_rows_b(z2), :], rb.at[chunk(j), ours, :], b1_s, b1_r.at[j], 2 * z2 + 1
            )

        @pl.when(c == 1)
        def _():
            here(dens.at[chunk(j), z_rows_b(z), :], rb.at[chunk(j), ours, :], b1_r.at[j])

        @pl.when(c == 0)
        def _():
            to_grid(
                dens.at[chunk(j), z_rows_b(z), :], rb.at[chunk(j), ours, :], b1_s, b1_r.at[j], 2 * z + 1
            )

    here(dens.at[last, pl.ds(0, 16), :], ra.at[last], a1_r.at[CHUNKS - 1])

    for j in range(CHUNKS):
        arrived(ra.at[chunk(j)], a1_r.at[j])
        for z2 in z_peers:
            to_grid(ra.at[chunk(j), z_rows(z2), :], box.at[chunk(j), ours, :], a2_s, x_ra.at[j], 2 * z2)

        @pl.when(c == 0)
        def _():
            here(ra.at[chunk(j), z_rows(z), :], box.at[chunk(j), ours, :], x_ra.at[j])

        @pl.when(c == 1)
        def _():
            to_grid(ra.at[chunk(j), z_rows(z), :], box.at[chunk(j), ours, :], a2_s, x_ra.at[j], 2 * z)
            arrived(rb.at[chunk(j)], b1_r.at[j])
            for k in members(j):
                to_orb(rb.at[k], box.at[k], b2_s, x_rb.at[j], ahead(k))
            if j == CHUNKS - 1:
                here(rb.at[last], box.at[last], x_rb.at[j])

    for j in range(CHUNKS):

        @pl.when(c == 0)
        def _():
            arrived(box.at[chunk(j)], x_ra.at[j])

        @pl.when(c == 1)
        def _():
            arrived(box.at[chunk(j)], x_rb.at[j])

        for h in range(2):
            places = [j * CHUNK + h * 4 + n for n in range(4)]
            v = jnp.concatenate([box[k] for k in places], axis=1)
            high, low = split(v)
            w = dot(tx_ref[...], jnp.concatenate([high, low, high], axis=0))
            for n, k in enumerate(places):
                start = pl.multiple_of(behind(k) * NX, NX)
                mid[pl.ds(start, NX), :] = w[:, n * LANES : (n + 1) * LANES]

    low_half = iota((N_ORB, LANES), 1) < NZ

    def plane(kx):
        return pl.ds(kx, N_ORB, stride=NX)

    for n in range(NX // 4):
        evens, odds = [], []
        for kx in (4 * n, 4 * n + 2):
            v0, v1 = mid[plane(kx), :], mid[plane(kx + 1), :]
            evens.append(jnp.where(low_half, v0, pltpu.roll(v1, NZ, 1)))
            odds.append(jnp.where(low_half, pltpu.roll(v0, NZ, 1), v1))
        v = jnp.concatenate([jnp.concatenate(evens, axis=1), jnp.concatenate(odds, axis=1)], axis=0)
        high, low = split(v)
        spectrum = dot(tyf_ref[...], jnp.concatenate([high, low, high], axis=0))
        spectrum = spectrum * jnp.concatenate([green[2 * n], green[2 * n + 1]], axis=1)
        high, low = split(spectrum)
        w = dot(tyi_ref[...], jnp.concatenate([high, low, high], axis=0))
        for h, kx in enumerate((4 * n, 4 * n + 2)):
            part = w[:, h * LANES : (h + 1) * LANES]
            even, odd = part[:N_ORB], part[N_ORB:]
            mid[plane(kx), :] = jnp.where(low_half, even, pltpu.roll(odd, NZ, 1))
            mid[plane(kx + 1), :] = jnp.where(low_half, pltpu.roll(even, NZ, 1), odd)

    for j in range(CHUNKS):
        for h in range(2):
            places = [j * CHUNK + h * 4 + n for n in range(4)]
            v = jnp.concatenate(
                [mid[pl.ds(pl.multiple_of(behind(k) * NX, NX), NX), :] for k in places], axis=1
            )
            high, low = split(v)
            w = dot(tx_ref[...], jnp.concatenate([high, low, high], axis=0))
            for n, k in enumerate(places):
                pot[k] = w[:, n * LANES : (n + 1) * LANES]

        @pl.when(c == 0)
        def _():
            for z2 in z_peers:
                for core in range(2):
                    g2 = 2 * z2 + core
                    to_grid(
                        pot.at[chunk(j), pl.ds(2 * g2, 2), :], ra2.at[chunk(j), z_rows(z), :],
                        c1_s, c1_r.at[j], g2,
                    )
            to_grid(
                pot.at[chunk(j), pl.ds(2 * (2 * z + 1), 2), :], ra2.at[chunk(j), z_rows(z), :],
                c1_s, c1_r.at[j], 2 * z + 1,
            )
            here(pot.at[chunk(j), ours, :], ra2.at[chunk(j), z_rows(z), :], c1_r.at[j])

        @pl.when(c == 1)
        def _():
            for k in members(j):
                to_orb(pot.at[k], rb2.at[k], d1_s, d1_r.at[j], behind(k))
            if j == CHUNKS - 1:
                here(pot.at[last], rb2.at[last], d1_r.at[j])

    for j in range(CHUNKS):
        arrived(ra2.at[chunk(j)], c1_r.at[j])
        for k in members(j):
            to_orb(ra2.at[k], back.at[k, pl.ds(0, 16), :], c2_s, c2_r.at[j], behind(k))
        if j == CHUNKS - 1:
            here(ra2.at[last], back.at[last, pl.ds(0, 16), :], c2_r.at[j])

        @pl.when(c == 1)
        def _():
            arrived(rb2.at[chunk(j)], d1_r.at[j])
            for z2 in z_peers:
                for core in range(2):
                    g2 = 2 * z2 + core
                    to_grid(
                        rb2.at[chunk(j), pl.ds(2 * g2, 2), :], back.at[chunk(j), z_rows_b(z), :],
                        d2_s, d2_r.at[j], g2,
                    )
            to_grid(
                rb2.at[chunk(j), pl.ds(2 * (2 * z), 2), :], back.at[chunk(j), z_rows_b(z), :],
                d2_s, d2_r.at[j], 2 * z,
            )
            here(rb2.at[chunk(j), ours, :], back.at[chunk(j), z_rows_b(z), :], d2_r.at[j])

    total = jnp.zeros((256, 2 * LANES), f32)
    for j in range(CHUNKS):
        arrived(back.at[chunk(j), pl.ds(0, 16), :], c2_r.at[j])
        arrived(back.at[chunk(j), pl.ds(16, 16), :], d2_r.at[j])
        rows = pl.ds(j * PREP, PREP)
        potential = z_product(back[chunk(j)].reshape(PREP, LANES), tz_ref[...])
        products = jnp.concatenate(split(potential * rot_j[rows, :]), axis=1)
        total = total + dot(sel_t[j], products)
    term[...] = (-(total[:, :LANES] + total[:, LANES:])).reshape(N_ORB, 8, LANES)

    for k in others:
        to_orb(term.at[ahead(k)], gathered.at[:, cells(o)], e4_s, e4_r, ahead(k))
    here(term.at[o], gathered.at[:, cells(o)], e4_r)

    most = pl.ds(0, N_ORB - 1)
    arrived(got.at[most], e1_s)
    arrived(ra.at[most], a1_s)
    arrived(term.at[most], e4_s)
    arrived(ra2.at[most], c2_s)

    @pl.when(c == 0)
    def _():
        arrived(rb.at[:, pl.ds(0, 16), :], b1_s)
        arrived(ra.at[:, pl.ds(0, 14), :], a2_s)
        arrived(pot.at[:, pl.ds(0, 30), :], c1_s)

    @pl.when(c == 1)
    def _():
        arrived(rb.at[:, pl.ds(0, 14), :], b1_s)
        arrived(ra.at[:, pl.ds(0, 16), :], a2_s)
        arrived(rb.at[most], b2_s)
        arrived(pot.at[most], d1_s)
        arrived(rb2.at[:, pl.ds(0, 30), :], d2_s)

    arrived(gathered, e4_r)
    stores = [
        (gathered.at[pl.ds(2 * n, 2), :], out_ref.at[n], out_sem.at[n]) for n in range(4)
    ]
    for args in stores:
        pltpu.make_async_copy(*args).start()
    for args in stores:
        pltpu.make_async_copy(*args).wait()


def on_device(orbitals, rotation, tile_list, pair_mask):
    consts = [jnp.asarray(t) for t in tables()]
    anyspace = pl.BlockSpec(memory_space=pl.ANY)
    dma = pltpu.SemaphoreType.DMA
    box = pltpu.VMEM((N_ORB, NX, LANES), f32)
    half_box = pltpu.VMEM((N_ORB, 16, LANES), f32)
    operands = [rotation, tile_list.T, pair_mask, *consts]
    return pl.pallas_call(
        kernel,
        out_shape=jax.ShapeDtypeStruct(orbitals.shape, f32),
        in_specs=[anyspace] * (4 + len(consts)),
        out_specs=anyspace,
        scratch_shapes=[pltpu.VMEM(a.shape, a.dtype) for a in operands]
        + [
            pltpu.VMEM((8, NY * NZ), f32),
            pltpu.VMEM((N_ORB, 8, LANES), f32),
            pltpu.VMEM((ROWS, 256), bf16),
            pltpu.VMEM((ROWS, 256), bf16),
            pltpu.VMEM((ROWS // PREP, 256, PREP), bf16),
            pltpu.VMEM((2, 256, 256), bf16),
            pltpu.VMEM((ROWS, LANES), f32),
            pltpu.VMEM((NX // 2, NY, LANES), f32),
            box,
            half_box,
            box,
            box,
            pltpu.VMEM((N_ORB * NX, LANES), f32),
            box,
            half_box,
            box,
            box,
            pltpu.VMEM((N_ORB, 8, LANES), f32),
            pltpu.VMEM((8, NY * NZ), f32),
            dma((4,)),
            dma((4,)),
            dma((len(operands),)),
        ]
        + [dma((CHUNKS,))] * 8
        + [dma] * 12,
        compiler_params=pltpu.CompilerParams(
            collective_id=0, has_side_effects=True, vmem_limit_bytes=67_000_000
        ),
    )(orbitals, *operands)


def solution(mesh):
    in_specs = (P("orb", "grid", None), P(), P(), P())
    out_specs = P("orb", "grid", None)
    return jax.shard_map(
        on_device, mesh=mesh, in_specs=in_specs, out_specs=out_specs, check_vma=False
    )
```

```python
import numpy as np
import jax
import jax.numpy as jnp
from jax import lax
from jax.experimental import pallas as pl
from jax.experimental.pallas import tpu as pltpu
from jax.sharding import PartitionSpec as P

NORB = 128
NX = 32
NY = 64
NZ = 64
NPAIR = 1024
LANES = 128
N_ORB = 32
N_GRID = 16
XDIM = 4
YDIM = 8
ZDIM = 8
CHUNKS = 4
CHUNK = 8
PEERS = sorted(
    ((dx, dy) for dx in (2, 1, -1, 0) for dy in (4, 3, -3, 2, -2, 1, -1, 0)),
    key=lambda step: -abs(step[0]) - abs(step[1]),
)
Z_STEPS = (4, 3, -3, 2, -2, 1, -1)
ROWS = 1024
PREP = 256
coupling = 0.25
screening = 0.1
MESH = pl.DeviceIdType.MESH
f32 = jnp.float32
bf16 = jnp.bfloat16


def sine_table(length):
    k = np.arange(length, dtype=np.float64) + 1.0
    return np.sqrt(2.0 / (length + 1.0)) * np.sin(np.pi * k[:, None] * k[None, :] / (length + 1.0))


def eigen_values(length):
    k = np.arange(length, dtype=np.float64) + 1.0
    return 2.0 - 2.0 * np.cos(np.pi * k / (length + 1.0))


def halves(table):
    high = table.astype(np.float32).astype(jnp.bfloat16)
    low = (table - high.astype(np.float64)).astype(np.float32).astype(jnp.bfloat16)
    return high, low


def tables():
    sx_h, sx_l = halves(sine_table(NX))
    table_x = np.concatenate([sx_h, sx_h, sx_l], axis=1)
    s = sine_table(NY)
    split_cols = np.concatenate([s[:, 0::2], s[:, 1::2]], axis=1)
    fh, fl = halves(split_cols)
    table_yf = np.concatenate([fh, fh, fl], axis=1)
    ih, il = halves(split_cols.T)
    table_yi = np.concatenate([ih, ih, il], axis=1)
    block = np.kron(np.eye(2), sine_table(NZ))
    bh, bl = halves(block)
    table_z = np.concatenate([bh, bl], axis=1)
    ly, lz, lx = eigen_values(NY), eigen_values(NZ), eigen_values(NX)
    sum_yz = ly[:, None] + np.tile(lz, 2)[None, :] + screening
    sum_x = np.repeat(lx.reshape(NX // 2, 2), NZ, axis=1)
    return (
        table_x,
        table_yf,
        table_yi,
        table_z,
        sum_yz.astype(np.float32),
        sum_x.astype(np.float32),
    )


def split(v):
    high = v.astype(bf16)
    low = (v - high.astype(f32)).astype(bf16)
    return high, low


def dot(a, b):
    return jnp.dot(a, b, preferred_element_type=f32)


def dot_nt(a, b):
    return lax.dot_general(a, b, (((1,), (1,)), ((), ())), preferred_element_type=f32)


def iota(shape, dim):
    return lax.broadcasted_iota(jnp.int32, shape, dim)


def one_hot(cond):
    return jnp.where(cond, 1.0, 0.0).astype(bf16)


def z_product(v, table_z):
    high, low = split(v)
    a = dot(high, table_z)
    return a[:, :LANES] + a[:, LANES:] + dot(low, table_z[:, :LANES])


def kernel(
    orb_hbm, rotation_hbm, tile_hbm, mask_hbm, tx_hbm, tyf_hbm, tyi_hbm, tz_hbm, syz_hbm, sx_hbm,
    out_ref,
    rotation_ref, tile_ref, mask_ref, tx_ref, tyf_ref, tyi_ref, tz_ref, syz_ref, sx_ref,
    own, got, sel_i, sel_j, sel_t, rot_k, rot_j, green, dens,
    ra, rb, box, mid, pot, ra2, rb2, back, term, gathered,
    in_sem, out_sem, table_sem,
    a1_r, b1_r, x_ra, x_rb, c1_r, d1_r, c2_r, d2_r,
    e1_r, e4_r, e1_s, a1_s, b1_s, a2_s, b2_s, c1_s, d1_s, c2_s, d2_s, e4_s,
):
    o = lax.axis_index("orb")
    g = lax.axis_index("grid")
    x, y = o // YDIM, o % YDIM
    z, c = g // 2, g % 2

    def ahead(k):
        dx, dy = PEERS[k]
        return (x + dx % XDIM) % XDIM * YDIM + (y + dy % YDIM) % YDIM

    def behind(k):
        dx, dy = PEERS[k]
        return (x + -dx % XDIM) % XDIM * YDIM + (y + -dy % YDIM) % YDIM

    def chunk(j):
        return pl.ds(j * CHUNK, CHUNK)

    def members(j):
        return range(j * CHUNK, min((j + 1) * CHUNK, N_ORB - 1))

    others = range(N_ORB - 1)
    z_peers = [(z + step % ZDIM) % ZDIM for step in Z_STEPS]

    def to_orb(src, dst, s_sem, r_sem, o2):
        pltpu.make_async_remote_copy(
            src_ref=src, dst_ref=dst, send_sem=s_sem, recv_sem=r_sem,
            device_id=(o2, g), device_id_type=MESH,
        ).start()

    def to_grid(src, dst, s_sem, r_sem, g2):
        pltpu.make_async_remote_copy(
            src_ref=src, dst_ref=dst, send_sem=s_sem, recv_sem=r_sem,
            device_id=(o, g2), device_id_type=MESH,
        ).start()

    def here(src, dst, r_sem):
        pltpu.make_async_copy(src, dst, r_sem).start()

    def arrived(ref, sem):
        pltpu.make_async_copy(ref, ref, sem).wait()

    loads = [
        (orb_hbm.at[n], own.at[pl.ds(2 * n, 2), :], in_sem.at[n]) for n in range(4)
    ]
    fetches = [
        (tile_hbm, tile_ref), (mask_hbm, mask_ref), (rotation_hbm, rotation_ref),
        (syz_hbm, syz_ref), (sx_hbm, sx_ref), (tz_hbm, tz_ref),
        (tx_hbm, tx_ref), (tyf_hbm, tyf_ref), (tyi_hbm, tyi_ref),
    ]
    barrier = pltpu.get_barrier_semaphore()
    for k in others:
        pl.semaphore_signal(barrier, inc=1, device_id=(ahead(k), g), device_id_type=MESH)
    for z2 in z_peers:
        for core in range(2):
            pl.semaphore_signal(barrier, inc=1, device_id=(o, 2 * z2 + core), device_id_type=MESH)
    pl.semaphore_signal(barrier, inc=1, device_id=(o, 2 * z + 1 - c), device_id_type=MESH)
    for args in loads:
        pltpu.make_async_copy(*args).start()
    for n, (src, dst) in enumerate(fetches):
        pltpu.make_async_copy(src, dst, table_sem.at[n]).start()
    for args in loads:
        pltpu.make_async_copy(*args).wait()
    pl.semaphore_wait(barrier, N_ORB - 1 + N_GRID - 1)

    def cells(o2):
        return pl.ds(pl.multiple_of(o2 * LANES, LANES), LANES)

    for k in others:
        to_orb(own.at[:, cells(ahead(k))], got.at[o], e1_s, e1_r, ahead(k))
    here(own.at[:, cells(o)], got.at[o], e1_r)

    for n, (src, dst) in enumerate(fetches):
        pltpu.make_async_copy(src, dst, table_sem.at[n]).wait()
    in_tile = one_hot(iota((64, NPAIR), 1) // 16 == iota((64, NPAIR), 0))
    corners = 4.0 * dot(tile_ref[...].astype(f32).astype(bf16), in_tile)
    p_row = iota((1, NPAIR), 1)
    target = corners[0:1, :] + (p_row // 4 % 4).astype(f32)
    source = corners[1:2, :] + (p_row % 4).astype(f32)
    half = (iota((256, NPAIR), 0) // 2).astype(f32)
    hot_i = one_hot(half == target)
    hot_j = one_hot(half == source)
    orb_row = iota((NORB, NPAIR), 0).astype(f32)
    mask_of = dot(mask_ref[...].astype(f32).astype(bf16), one_hot(orb_row == source))
    live = jnp.sum(jnp.where(orb_row == target, mask_of, 0.0), axis=0, keepdims=True)
    before = one_hot(iota((LANES, LANES), 0) < iota((LANES, LANES), 1))
    every = jnp.ones((LANES, LANES), bf16)
    running = jnp.zeros((8, LANES), f32)
    ranks = []
    for n in range(NPAIR // LANES):
        flags = jnp.broadcast_to(live[:, n * LANES : (n + 1) * LANES], (8, LANES))
        bits = flags.astype(bf16)
        rank = dot(bits, before) + running
        running = running + dot(bits, every)
        ranks.append(jnp.where(flags > 0.5, rank, -1.0)[0:1, :])
    rank = jnp.concatenate(ranks, axis=1)

    same_plane = iota((PREP, 256), 0) % 2 == iota((PREP, 256), 1) % 2

    slot = (iota((32, NPAIR), 0) // 2).astype(f32)
    for j in range(CHUNKS):
        rows = pl.ds(j * PREP, PREP)
        parts = [
            one_hot(slot == rank - (16 * ahead(k)).astype(f32))
            for k in range(j * CHUNK, (j + 1) * CHUNK)
        ]
        chosen = jnp.concatenate(parts, axis=0)
        sel_i[rows, :] = jnp.where(same_plane, dot_nt(chosen, hot_i), 0.0).astype(bf16)
        sel_j[rows, :] = jnp.where(same_plane, dot_nt(chosen, hot_j), 0.0).astype(bf16)
        sel_t[j] = jnp.where(same_plane, dot_nt(hot_i, chosen), 0.0).astype(bf16)

    widen = one_hot(iota((256, NORB), 0) // 2 == iota((256, NORB), 1))
    widen_t = one_hot(iota((NORB, 256), 0) == iota((NORB, 256), 1) // 2)
    for n, part in enumerate(split(rotation_ref[...])):
        tall = dot_nt(widen, part).astype(bf16)
        rot_k[n] = jnp.where(same_plane, dot(tall, widen_t), 0.0).astype(bf16)

    def fill_green(n, carry):
        green[n] = coupling / (syz_ref[...] + sx_ref[pl.ds(n, 1), :])
        return carry

    lax.fori_loop(0, NX // 2, fill_green, 0)

    arrived(got, e1_r)

    got_h, got_l = split(got[...].reshape(256, LANES))
    wide = dot(rot_k[0], jnp.concatenate([got_h, got_l], axis=1))
    rotated = wide[:, :LANES] + wide[:, LANES:] + dot(rot_k[1], got_h)
    rotated = jnp.concatenate(split(rotated), axis=1)

    def density_rows(j, h):
        rows = pl.ds(j * PREP + h * 128, 128)
        wide_i = dot(sel_i[rows, :], rotated)
        wide_j = dot(sel_j[rows, :], rotated)
        at_j = wide_j[:, :LANES] + wide_j[:, LANES:]
        rot_j[rows, :] = at_j
        density = (wide_i[:, :LANES] + wide_i[:, LANES:]) * at_j
        spectrum = z_product(density, tz_ref[...])
        dens[pl.ds(j * CHUNK + h * 4, 4)] = spectrum.reshape(4, 32, LANES)

    ours = pl.ds(2 * g, 2)

    def z_rows(z2):
        return pl.ds(2 * z2, 2)

    def z_rows_b(z2):
        return pl.ds(16 + 2 * z2, 2)

    last = N_ORB - 1
    for j in range(CHUNKS):
        for h in range(2):
            density_rows(j, h)
            for k in members(j)[h * 4 : h * 4 + 4]:
                to_orb(dens.at[k, pl.ds(0, 16), :], ra.at[k], a1_s, a1_r.at[j], ahead(k))
        for z2 in z_peers:
            to_grid(
                dens.at[chunk(j), z_rows_b(z2), :], rb.at[chunk(j), ours, :], b1_s, b1_r.at[j], 2 * z2 + 1
            )

        @pl.when(c == 1)
        def _():
            here(dens.at[chunk(j), z_rows_b(z), :], rb.at[chunk(j), ours, :], b1_r.at[j])

        @pl.when(c == 0)
        def _():
            to_grid(
                dens.at[chunk(j), z_rows_b(z), :], rb.at[chunk(j), ours, :], b1_s, b1_r.at[j], 2 * z + 1
            )

    here(dens.at[last, pl.ds(0, 16), :], ra.at[last], a1_r.at[CHUNKS - 1])

    for j in range(CHUNKS):
        arrived(ra.at[chunk(j)], a1_r.at[j])
        for z2 in z_peers:
            to_grid(ra.at[chunk(j), z_rows(z2), :], box.at[chunk(j), ours, :], a2_s, x_ra.at[j], 2 * z2)

        @pl.when(c == 0)
        def _():
            here(ra.at[chunk(j), z_rows(z), :], box.at[chunk(j), ours, :], x_ra.at[j])

        @pl.when(c == 1)
        def _():
            to_grid(ra.at[chunk(j), z_rows(z), :], box.at[chunk(j), ours, :], a2_s, x_ra.at[j], 2 * z)
            arrived(rb.at[chunk(j)], b1_r.at[j])
            for k in members(j):
                to_orb(rb.at[k], box.at[k], b2_s, x_rb.at[j], ahead(k))
            if j == CHUNKS - 1:
                here(rb.at[last], box.at[last], x_rb.at[j])

    for j in range(CHUNKS):

        @pl.when(c == 0)
        def _():
            arrived(box.at[chunk(j)], x_ra.at[j])

        @pl.when(c == 1)
        def _():
            arrived(box.at[chunk(j)], x_rb.at[j])

        for h in range(2):
            places = [j * CHUNK + h * 4 + n for n in range(4)]
            v = jnp.concatenate([box[k] for k in places], axis=1)
            high, low = split(v)
            w = dot(tx_ref[...], jnp.concatenate([high, low, high], axis=0))
            for n, k in enumerate(places):
                start = pl.multiple_of(behind(k) * NX, NX)
                mid[pl.ds(start, NX), :] = w[:, n * LANES : (n + 1) * LANES]

    low_half = iota((N_ORB, LANES), 1) < NZ

    def plane(kx):
        return pl.ds(kx, N_ORB, stride=NX)

    for n in range(NX // 4):
        evens, odds = [], []
        for kx in (4 * n, 4 * n + 2):
            v0, v1 = mid[plane(kx), :], mid[plane(kx + 1), :]
            evens.append(jnp.where(low_half, v0, pltpu.roll(v1, NZ, 1)))
            odds.append(jnp.where(low_half, pltpu.roll(v0, NZ, 1), v1))
        v = jnp.concatenate([jnp.concatenate(evens, axis=1), jnp.concatenate(odds, axis=1)], axis=0)
        high, low = split(v)
        spectrum = dot(tyf_ref[...], jnp.concatenate([high, low, high], axis=0))
        spectrum = spectrum * jnp.concatenate([green[2 * n], green[2 * n + 1]], axis=1)
        high, low = split(spectrum)
        w = dot(tyi_ref[...], jnp.concatenate([high, low, high], axis=0))
        for h, kx in enumerate((4 * n, 4 * n + 2)):
            part = w[:, h * LANES : (h + 1) * LANES]
            even, odd = part[:N_ORB], part[N_ORB:]
            mid[plane(kx), :] = jnp.where(low_half, even, pltpu.roll(odd, NZ, 1))
            mid[plane(kx + 1), :] = jnp.where(low_half, pltpu.roll(even, NZ, 1), odd)

    for j in range(CHUNKS):
        for h in range(2):
            places = [j * CHUNK + h * 4 + n for n in range(4)]
            v = jnp.concatenate(
                [mid[pl.ds(pl.multiple_of(behind(k) * NX, NX), NX), :] for k in places], axis=1
            )
            high, low = split(v)
            w = dot(tx_ref[...], jnp.concatenate([high, low, high], axis=0))
            for n, k in enumerate(places):
                pot[k] = w[:, n * LANES : (n + 1) * LANES]

        @pl.when(c == 0)
        def _():
            for z2 in z_peers:
                for core in range(2):
                    g2 = 2 * z2 + core
                    to_grid(
                        pot.at[chunk(j), pl.ds(2 * g2, 2), :], ra2.at[chunk(j), z_rows(z), :],
                        c1_s, c1_r.at[j], g2,
                    )
            to_grid(
                pot.at[chunk(j), pl.ds(2 * (2 * z + 1), 2), :], ra2.at[chunk(j), z_rows(z), :],
                c1_s, c1_r.at[j], 2 * z + 1,
            )
            here(pot.at[chunk(j), ours, :], ra2.at[chunk(j), z_rows(z), :], c1_r.at[j])

        @pl.when(c == 1)
        def _():
            for k in members(j):
                to_orb(pot.at[k], rb2.at[k], d1_s, d1_r.at[j], behind(k))
            if j == CHUNKS - 1:
                here(pot.at[last], rb2.at[last], d1_r.at[j])

    for j in range(CHUNKS):
        @pl.when(c == 1)
        def _():
            arrived(rb2.at[chunk(j)], d1_r.at[j])
            for z2 in z_peers:
                for core in range(2):
                    g2 = 2 * z2 + core
                    to_grid(
                        rb2.at[chunk(j), pl.ds(2 * g2, 2), :], back.at[chunk(j), z_rows_b(z), :],
                        d2_s, d2_r.at[j], g2,
                    )
            to_grid(
                rb2.at[chunk(j), pl.ds(2 * (2 * z), 2), :], back.at[chunk(j), z_rows_b(z), :],
                d2_s, d2_r.at[j], 2 * z,
            )
            here(rb2.at[chunk(j), ours, :], back.at[chunk(j), z_rows_b(z), :], d2_r.at[j])

        arrived(ra2.at[chunk(j)], c1_r.at[j])
        for k in members(j):
            to_orb(ra2.at[k], back.at[k, pl.ds(0, 16), :], c2_s, c2_r.at[j], behind(k))
        if j == CHUNKS - 1:
            here(ra2.at[last], back.at[last, pl.ds(0, 16), :], c2_r.at[j])

    total = jnp.zeros((256, 2 * LANES), f32)
    for j in range(CHUNKS):
        arrived(back.at[chunk(j), pl.ds(0, 16), :], c2_r.at[j])
        arrived(back.at[chunk(j), pl.ds(16, 16), :], d2_r.at[j])
        rows = pl.ds(j * PREP, PREP)
        potential = z_product(back[chunk(j)].reshape(PREP, LANES), tz_ref[...])
        products = jnp.concatenate(split(potential * rot_j[rows, :]), axis=1)
        total = total + dot(sel_t[j], products)
    term[...] = (-(total[:, :LANES] + total[:, LANES:])).reshape(N_ORB, 8, LANES)

    for k in others:
        to_orb(term.at[ahead(k)], gathered.at[:, cells(o)], e4_s, e4_r, ahead(k))
    here(term.at[o], gathered.at[:, cells(o)], e4_r)

    most = pl.ds(0, N_ORB - 1)
    arrived(got.at[most], e1_s)
    arrived(ra.at[most], a1_s)
    arrived(term.at[most], e4_s)
    arrived(ra2.at[most], c2_s)

    @pl.when(c == 0)
    def _():
        arrived(rb.at[:, pl.ds(0, 16), :], b1_s)
        arrived(ra.at[:, pl.ds(0, 14), :], a2_s)
        arrived(pot.at[:, pl.ds(0, 30), :], c1_s)

    @pl.when(c == 1)
    def _():
        arrived(rb.at[:, pl.ds(0, 14), :], b1_s)
        arrived(ra.at[:, pl.ds(0, 16), :], a2_s)
        arrived(rb.at[most], b2_s)
        arrived(pot.at[most], d1_s)
        arrived(rb2.at[:, pl.ds(0, 30), :], d2_s)

    arrived(gathered, e4_r)
    stores = [
        (gathered.at[pl.ds(2 * n, 2), :], out_ref.at[n], out_sem.at[n]) for n in range(4)
    ]
    for args in stores:
        pltpu.make_async_copy(*args).start()
    for args in stores:
        pltpu.make_async_copy(*args).wait()


def on_device(orbitals, rotation, tile_list, pair_mask):
    consts = [jnp.asarray(t) for t in tables()]
    anyspace = pl.BlockSpec(memory_space=pl.ANY)
    dma = pltpu.SemaphoreType.DMA
    box = pltpu.VMEM((N_ORB, NX, LANES), f32)
    half_box = pltpu.VMEM((N_ORB, 16, LANES), f32)
    operands = [rotation, tile_list.T, pair_mask, *consts]
    return pl.pallas_call(
        kernel,
        out_shape=jax.ShapeDtypeStruct(orbitals.shape, f32),
        in_specs=[anyspace] * (4 + len(consts)),
        out_specs=anyspace,
        scratch_shapes=[pltpu.VMEM(a.shape, a.dtype) for a in operands]
        + [
            pltpu.VMEM((8, NY * NZ), f32),
            pltpu.VMEM((N_ORB, 8, LANES), f32),
            pltpu.VMEM((ROWS, 256), bf16),
            pltpu.VMEM((ROWS, 256), bf16),
            pltpu.VMEM((ROWS // PREP, 256, PREP), bf16),
            pltpu.VMEM((2, 256, 256), bf16),
            pltpu.VMEM((ROWS, LANES), f32),
            pltpu.VMEM((NX // 2, NY, LANES), f32),
            box,
            half_box,
            box,
            box,
            pltpu.VMEM((N_ORB * NX, LANES), f32),
            box,
            half_box,
            box,
            box,
            pltpu.VMEM((N_ORB, 8, LANES), f32),
            pltpu.VMEM((8, NY * NZ), f32),
            dma((4,)),
            dma((4,)),
            dma((len(operands),)),
        ]
        + [dma((CHUNKS,))] * 8
        + [dma] * 12,
        compiler_params=pltpu.CompilerParams(
            collective_id=0, has_side_effects=True, vmem_limit_bytes=67_000_000
        ),
    )(orbitals, *operands)


def solution(mesh):
    in_specs = (P("orb", "grid", None), P(), P(), P())
    out_specs = P("orb", "grid", None)
    return jax.shard_map(
        on_device, mesh=mesh, in_specs=in_specs, out_specs=out_specs, check_vma=False
    )
```
